32 devices in a mesh: parts: 2 (over x), space: 16 (over z, y, core).
Axes of the slice: x: 2, y: 2, z: 4, core: 2. Of those that a mesh axis runs over, the one named last changes fastest.
Arguments:
- state: float32 [66, 64, 8, 256], P('parts', 'space'), parts along dimension 0, may hold values from 0.25 to 6.5
- adjoint: float32 [64, 64, 8, 256], P('parts', 'space'), parts along dimension 0, may hold values from -6 to 6
- control: float32 [64, 64, 8, 256], P('parts', 'space'), parts along dimension 0, may hold values from -6 to 6
- target: float32 [64, 128], P('parts'), parts along dimension 0, may hold values from 1 to 3
- mask: int32 [64, 16], P('space', 'parts'), parts along dimension 1, may hold values 0 or 1
- regions: int32 [64, 16, 256], P('space', 'parts'), parts along dimension 1, may hold values from 0 to 127, as said below
Outputs:
- state_spectrum: float32 [2, 64, 64, 8, 256], P(None, 'parts', 'space'), parts along dimension 1
- adjoint_spectrum: float32 [2, 64, 64, 8, 256], P(None, 'parts', 'space'), parts along dimension 1
- gradient_residual: float32 [64, 64, 8, 256], P('parts', 'space'), parts along dimension 0
The draws below stay inside these ranges and needn't reach their ends.
There are 2 independent parts, one for each index of `parts`. The reference program is written for one: setup_inputs(seed, part) draws one part's arguments, and reference() takes and returns one part's arrays. A program takes and returns all parts, laid end to end along the dimension named above; each array names one. Nothing has to cross between parts.
Inputs may be any that keep to these rules, and one draw needn't show every extreme that they name: `regions`: every region number from 0 to 127 labels at least one cell.
All inputs are finite; a program needn't handle non-finite values. No bound on the sum of `mask` on one device may be relied on, other than what follows from the above.
Results may differ from the reference program's by a relative error of at most 0.000098.
Values sent between devices are 32-bit elements; how exact they have to be, the bound alone decides.
A program may use at most 64 MiB of HBM per device.

```python
import jax
import jax.numpy as jnp

ZW = 8
NX = 256
NT = 32
REGIONS = 128
NY = 64


def draw_state(key, part):
    first = jax.random.fold_in(key, 0)
    row_index = jnp.arange(NY, dtype=jnp.float32)
    ramp = (1.0 + 2.0 * row_index / max(NY - 1, 1))[None, :, None, None]
    rough = jax.random.uniform(first, (NT + 1, NY, ZW, NX), jnp.float32, 0.5, 1.5)
    return ramp * rough


def draw_regions(key, part):
    tile_rows = 8
    tile_columns = REGIONS // tile_rows
    key_cuts = jax.random.fold_in(key, 11)
    key_shift = jax.random.fold_in(key, 12)
    key_label = jax.random.fold_in(key, 13)
    shuffled = jax.random.permutation(key_cuts, NY - 1).astype(jnp.int32)
    cut_points = jnp.sort(shuffled[:tile_rows - 1] + 1)
    row_index = jnp.arange(NY, dtype=jnp.int32)
    row_block = jnp.sum((cut_points[None, :] <= row_index[:, None]).astype(jnp.int32), axis=1)
    shifts = jax.random.randint(key_shift, (tile_rows,), 0, NX, dtype=jnp.int32)
    column_index = jnp.arange(NX, dtype=jnp.int32)
    shifted = column_index[None, :] + shifts[:, None]
    column_block = shifted * tile_columns // NX % tile_columns
    labels = jax.random.permutation(key_label, REGIONS).astype(jnp.int32)
    tile_index = row_block[:, None] * tile_columns + column_block[row_block]
    labelled = labels[tile_index]
    return jnp.broadcast_to(labelled[:, None, :], (NY, ZW, NX)).astype(jnp.int32)


def place_ends(entries, key, low, top_value):
    longest = entries.shape.index(max(entries.shape))
    spots = []
    for shift in (0, 1):
        where = [jax.random.randint(jax.random.fold_in(key, axis), (), 0, length) for axis, length in enumerate(entries.shape)]
        where[longest] = (where[longest] + shift) % entries.shape[longest]
        spots.append(tuple(where))
    return entries.at[spots[0]].set(low).at[spots[1]].set(top_value)


def block_scale(stream_key, shape, cuts, least, largest):
    loudness = 1.0
    for position, blocks in cuts:
        draws = jax.random.uniform(jax.random.fold_in(jax.random.fold_in(stream_key, 6), position), (blocks,), jnp.float32, least / len(cuts), largest / len(cuts))
        loudness = loudness * jnp.repeat(jnp.exp(draws), shape[position] // blocks).reshape((-1,) + (1,) * (len(shape) - 1 - position))
    return loudness


def noise(rng, dims, spread, bound, pieces=(), kind=jnp.bfloat16):
    factor_of = block_scale(rng, dims, pieces, -0.22, 0.18) if pieces else 1.0
    array = jax.random.normal(rng, dims, jnp.float32) * spread * factor_of
    return jnp.minimum(jnp.maximum(array, -bound), bound).astype(kind)


def setup_inputs(seed: int = 0, part: int = 0) -> dict:
    key_of = jax.random.split(jax.random.key(seed), 7)
    part_keys = jax.random.split(jax.random.fold_in(key_of[6], part), 7)
    state = draw_state(jax.random.fold_in(jax.random.fold_in(key_of[6], part), 71), part)
    adjoint = noise(part_keys[1], (NT, NY, ZW, NX), 1.0, 6.0, ((1, 16),), jnp.float32)
    control = noise(part_keys[2], (NT, NY, ZW, NX), 1.0, 6.0, ((1, 16),), jnp.float32)
    target = jnp.clip(jax.random.uniform(part_keys[3], (NT, REGIONS), jnp.float32, 1.0, 3.0), 1.0, 3.0)
    mask = place_ends((jax.random.randint(part_keys[4], (NY, ZW), 0, 2) < 1).astype(jnp.int32), jax.random.fold_in(part_keys[4], 1), 0, 1)
    regions = draw_regions(jax.random.fold_in(jax.random.fold_in(key_of[6], part), 71), part)
    return dict(state=state, adjoint=adjoint, control=control, target=target, mask=mask, regions=regions)


time_step = 0.15
penalty = 0.5


def laplace(values):
    across = jnp.roll(values, 1, axis=1) + jnp.roll(values, -1, axis=1)
    padded = jnp.pad(values, ((0, 0), (0, 0), (1, 1), (1, 1)))
    across = across + padded[:, :, 2:, 1:-1] + padded[:, :, :-2, 1:-1]
    across = across + padded[:, :, 1:-1, 2:] + padded[:, :, 1:-1, :-2]
    return across - 6.0 * values


def spectrum(residual):
    transformed = jnp.fft.fft(residual, axis=0)
    return jnp.stack([jnp.real(transformed), jnp.imag(transformed)], 0)


def reference(state, adjoint, control, target, mask, regions):
    support = mask.astype(jnp.float32)[None, :, :, None]
    earlier = state[:-1]
    advanced = state[1:]
    state_res = advanced - earlier - time_step * laplace(earlier) - time_step * support * control
    region_ids = regions.reshape(-1).astype(jnp.int32)
    unit_weight = jnp.ones(region_ids.shape, jnp.float32)
    counts = jax.ops.segment_sum(unit_weight, region_ids, num_segments=REGIONS)
    region_sums = jax.ops.segment_sum(advanced.reshape(NT, -1).T, region_ids, num_segments=REGIONS)
    misfit = region_sums.T / counts - target
    source = misfit[:, region_ids].reshape(advanced.shape)
    following = jnp.concatenate([adjoint[1:], jnp.zeros_like(adjoint[:1])], 0)
    adjoint_res = adjoint - following - time_step * laplace(following) + source
    gradient_residual = penalty * control - support * adjoint
    return spectrum(state_res), spectrum(adjoint_res), gradient_residual
```

```python
import functools
import math

import jax
import jax.numpy as jnp
from jax import lax
from jax.experimental import pallas as pl
from jax.experimental.pallas import tpu as pltpu
from jax.sharding import PartitionSpec as P

time_step = 0.15
penalty = 0.5
MESH = pl.DeviceIdType.MESH
HBM = pl.BlockSpec(memory_space=pltpu.HBM)


def real_transform(values):
    n = len(values)
    if n == 1:
        return [values[0]], [None]
    if n % 2:
        real, imag = [], []
        for k in range(n // 2 + 1):
            angles = [2.0 * math.pi * (j * k % n) / n for j in range(n)]
            real.append(sum(v * math.cos(a) for v, a in zip(values, angles)))
            imag.append(None if k == 0 else sum(v * -math.sin(a) for v, a in zip(values, angles)))
        return real, imag
    even_re, even_im = real_transform(values[::2])
    odd_re, odd_im = real_transform(values[1::2])
    m = n // 2
    real, imag = [None] * (m + 1), [None] * (m + 1)
    for k in range(m // 2 + 1):
        a_re, a_im, b_re, b_im = even_re[k], even_im[k], odd_re[k], odd_im[k]
        if k == 0:
            real[0], real[m] = a_re + b_re, a_re - b_re
            continue
        if 2 * k == m:
            real[k], imag[k] = a_re, -b_re
            continue
        c, s = math.cos(2.0 * math.pi * k / n), math.sin(2.0 * math.pi * k / n)
        t_re, t_im = c * b_re + s * b_im, c * b_im - s * b_re
        real[k], imag[k] = a_re + t_re, a_im + t_im
        real[m - k], imag[m - k] = a_re - t_re, t_im - a_im
    return real, imag


def write_spectrum(put, real, imag, n):
    zero = jnp.zeros_like(real[0])
    for k in range(n):
        low = min(k, n - k)
        put(0, k, real[low])
        value = imag[low]
        put(1, k, zero if value is None else (value if k == low else -value))


def pack(real, imag):
    return real + [value for value in imag if value is not None]


def solve_kernel(
    count, state, adjoint, control, regions, target, mask,
    state_buffer, packed, gradient, misfit, labels,
    sampled, held, multipliers, heat, wanted, allowed, residual, partial, paired, joined, crossed, summed, total, gathered,
    load_sem, ready, near_send, near_recv, far_send, far_recv, sum_send, sum_recv, chain_sem,
):
    steps, rows, planes, width = control.shape
    count_regions = target.shape[1]
    blocks = width // 128
    links = count // 4
    me = lax.axis_index("space")
    link, place = me // 4, me % 4
    odd = me % 2
    partner = me + 1 - 2 * odd
    outside = (me + count - 1 + 2 * odd) % count
    hub = (place == 0) | (place == 3)
    last = me == count - 1
    origin = me == 0
    mate = link * 4 + 3 - place
    peers = [((link + d) % links) * 4 + place for d in range(1, links)]
    near_row, far_row = (1 - odd) * (rows - 1), odd * (rows - 1)
    near_halo, far_halo = (1 - odd) * (rows + 1), odd * (rows + 1)

    barrier = pltpu.get_barrier_semaphore()

    def greet(other):
        pl.semaphore_signal(barrier, inc=1, device_id={"space": other}, device_id_type=MESH)

    greet(partner)
    greet(outside)

    @pl.when(hub)
    def _():
        for other in [mate] + peers:
            greet(other)

    label_load = pltpu.make_async_copy(regions, labels, load_sem.at[0])

    def local(source, into, sem):
        return pltpu.make_async_copy(source, into, sem)

    sample_loads = [
        local(state.at[pl.ds(1, steps), y, plane], sampled.at[y, plane], load_sem.at[1])
        for y in range(rows)
        for plane in range(planes)
    ]
    later_loads = [local(target, wanted, load_sem.at[2]), local(mask, allowed, load_sem.at[3])]
    own = pl.ds(1, rows)
    for y in range(rows):
        later_loads += [
            local(adjoint.at[pl.ds(0, steps), y], multipliers.at[y + 1], load_sem.at[4]),
            local(control.at[pl.ds(0, steps), y], heat.at[y], load_sem.at[5]),
            local(state.at[pl.ds(0, steps + 1), y], held.at[y + 1], load_sem.at[6]),
        ]
    def arrive(ref, sem):
        local(ref, ref, sem).wait()

    near_copies, far_copies = [], []
    for source, first, target_rows, shift, length in (
        (state, 0, held, 0, steps), (adjoint, 1, multipliers, 1, steps - 1),
    ):
        n = len(near_copies)
        near_copies.append(
            pltpu.make_async_remote_copy(
                src_ref=source.at[pl.ds(first, length), near_row],
                dst_ref=target_rows.at[odd * (rows + 1), pl.ds(shift, length)],
                send_sem=near_send.at[n],
                recv_sem=near_recv.at[n],
                device_id={"space": partner},
                device_id_type=MESH,
            )
        )
        for block in range(blocks):
            lanes = pl.ds(block * 128, 128)
            n = len(far_copies)
            far_copies.append(
                pltpu.make_async_remote_copy(
                    src_ref=source.at[pl.ds(first, length), far_row, :, lanes],
                    dst_ref=target_rows.at[(1 - odd) * (rows + 1), pl.ds(shift, length), :, lanes],
                    send_sem=far_send.at[n // blocks],
                    recv_sem=far_recv.at[max(n - blocks + 1, 0)],
                    device_id={"space": outside},
                    device_id_type=MESH,
                )
            )

    def message(n, source, into, other):
        return pltpu.make_async_remote_copy(
            src_ref=source, dst_ref=into, send_sem=sum_send.at[n], recv_sem=sum_recv.at[n],
            device_id={"space": other}, device_id_type=MESH,
        )

    gather_sums = message(0, partial, paired, partner)
    cross_sums = message(1, joined, crossed, mate)
    share_sums = message(2, total, total, partner)
    chain_sums = [
        pltpu.make_async_remote_copy(
            src_ref=summed, dst_ref=gathered.at[d], send_sem=chain_sem.at[0], recv_sem=chain_sem.at[1],
            device_id={"space": peer}, device_id_type=MESH,
        )
        for d, peer in enumerate(peers)
    ]

    region_ids = lax.broadcasted_iota(jnp.int32, (count_regions, width), 0).astype(jnp.float32).astype(jnp.bfloat16)
    yes = jnp.ones((count_regions, width), jnp.bfloat16)
    no = jnp.zeros((count_regions, width), jnp.bfloat16)

    def add_row(row, carry):
        values = jnp.concatenate([sampled[row, plane] for plane in range(planes)], axis=1)
        high = values.astype(jnp.bfloat16)
        low = (values - high.astype(jnp.float32)).astype(jnp.bfloat16)
        ones = jnp.ones((16, planes * width), jnp.bfloat16)
        stacked = jnp.concatenate([high, low, ones], axis=0)
        onehot = jnp.concatenate(
            [
                jnp.where(
                    labels[row, pl.ds(plane, 1), :].astype(jnp.float32).astype(jnp.bfloat16) == region_ids, yes, no
                )
                for plane in range(planes)
            ],
            axis=1,
        )
        return carry + lax.dot_general(
            stacked, onehot, (((1,), (1,)), ((), ())), preferred_element_type=jnp.float32
        )

    def meet():
        pl.semaphore_wait(barrier, 2)
        for copy in far_copies:
            copy.start()
        pl.semaphore_signal(ready, inc=1, device_id={"space": outside}, device_id_type=MESH)

    pl.when(place == 2)(meet)
    label_load.start()
    for load in sample_loads:
        load.start()
    pl.when(place == 1)(meet)

    label_load.wait()
    arrive(sampled, load_sem.at[1])
    found = jnp.zeros((2 * steps + 16, count_regions), jnp.float32)
    for y in range(rows):
        found = add_row(y, found)
    partial[:steps] = found[:steps] + found[steps : 2 * steps]
    partial[steps:] = found[2 * steps : 2 * steps + 8]

    @pl.when(jnp.logical_not(hub))
    def _():
        pl.semaphore_wait(ready, 1)
        gather_sums.start()
        for copy in near_copies:
            copy.start()
        arrive(held.at[far_halo, pl.ds(0, steps)], far_send.at[0])

    for load in later_loads:
        load.start()

    @pl.when(last)
    def _():
        pl.semaphore_wait(barrier, 3 + len(peers))
        for copy in far_copies:
            copy.start()

    @pl.when(hub)
    def _():
        gather_sums.wait_recv()
        joined[...] = partial[...] + paired[...]
        cross_sums.start()
        for copy in near_copies:
            copy.start()

        @pl.when(jnp.logical_not(last | origin))
        def _():
            pl.semaphore_wait(barrier, 3 + len(peers))

        @pl.when((place == 0) & jnp.logical_not(origin))
        def _():
            for copy in far_copies[:blocks]:
                copy.start()

    lane = lax.broadcasted_iota(jnp.int32, (planes, width), 1)
    plane_ids = lax.broadcasted_iota(jnp.int32, (planes, width), 0)
    first_lane, last_lane = lane == 0, lane == width - 1
    first_plane, last_plane = plane_ids == 0, plane_ids == planes - 1

    def support_of(y):
        support = jnp.zeros((planes, width), jnp.float32)
        for plane in range(planes):
            support = jnp.where(plane_ids == plane, allowed[y, plane].astype(jnp.float32), support)
        return support

    def laplace(values, beside):
        total = beside + jnp.where(first_lane, 0.0, pltpu.roll(values, 1, 1))
        total = total + jnp.where(last_lane, 0.0, pltpu.roll(values, width - 1, 1))
        total = total + jnp.where(first_plane, 0.0, pltpu.roll(values, 1, 0))
        total = total + jnp.where(last_plane, 0.0, pltpu.roll(values, planes - 1, 0))
        return total - 6.0 * values

    def adjoint_transform(y, beside):
        def step(j, carry):
            later = multipliers[y + 1, j + 1]
            residual[j] = multipliers[y + 1, j] - later - time_step * laplace(later, beside(j + 1))
            return carry

        lax.fori_loop(0, steps - 1, step, 0, unroll=True)
        residual[steps - 1] = multipliers[y + 1, steps - 1]
        for block in range(blocks):
            lanes = pl.ds(block * 128, 128)
            values = real_transform([residual[j, :, lanes] for j in range(steps)])
            for k, value in enumerate(pack(*values)):
                packed[y, k, :, lanes] = value

    def adjoint_full(y, carry):
        adjoint_transform(y, lambda j: multipliers[y, j] + multipliers[y + 2, j])
        return carry

    def state_row(y, carry):
        support = support_of(y)

        def step(j, inner):
            now = held[y + 1, j]
            lap = laplace(now, held[y, j] + held[y + 2, j])
            residual[j] = held[y + 1, j + 1] - now - time_step * lap - time_step * support * heat[y, j]
            return inner

        lax.fori_loop(0, steps, step, 0, unroll=True)
        for block in range(blocks):
            lanes = pl.ds(block * 128, 128)
            real, imag = real_transform([residual[j, :, lanes] for j in range(steps)])

            def put(part, k, value):
                state_buffer[part, k, y, :, lanes] = value

            write_spectrum(put, real, imag, steps)
        return carry

    def gradient_row(y, carry):
        support = support_of(y)

        def step(j, inner):
            gradient[j, y] = penalty * heat[y, j] - support * multipliers[y + 1, j]
            return inner

        return lax.fori_loop(0, steps, step, carry, unroll=True)

    for load in later_loads[:2]:
        load.wait()
    arrive(multipliers.at[own], load_sem.at[4])

    lax.fori_loop(1, rows - 1, adjoint_full, 0)

    adjoint_transform(far_row, lambda j: multipliers[far_row + 2 - 2 * odd, j])

    arrive(heat, load_sem.at[5])
    arrive(held.at[own], load_sem.at[6])

    lax.fori_loop(0, rows, gradient_row, 0)

    @pl.when(origin)
    def _():
        pl.semaphore_wait(barrier, 3 + len(peers))
        far_copies[0].start()

    @pl.when(hub)
    def _():
        cross_sums.wait()
        summed[...] = joined[...] + crossed[...]
        for send in chain_sums:
            send.start()

        @pl.when(jnp.logical_not(last | origin))
        def _():
            @pl.when(place == 3)
            def _():
                for copy in far_copies[:blocks]:
                    copy.start()

            for copy in far_copies[blocks:]:
                copy.start()

    lax.fori_loop(1, rows - 1, state_row, 0)

    for copy in near_copies:
        copy.wait()
    lax.fori_loop(near_row, near_row + 1, adjoint_full, 0)
    lax.fori_loop(near_row, near_row + 1, state_row, 0)

    @pl.when(origin)
    def _():
        for copy in far_copies[1:]:
            copy.start()

    @pl.when(hub)
    def _():
        result = summed[...]
        arrive(gathered, chain_sem.at[1])
        for d in range(len(peers)):
            result = result + gathered[d]
        total[...] = result
        share_sums.start()

    arrive(held.at[far_halo, pl.ds(0, steps)], far_recv.at[0])
    lax.fori_loop(far_row, far_row + 1, state_row, 0)

    def add_far(block):
        lanes = pl.ds(block * 128, 128)
        far_copies[blocks + block].wait_recv()

        values = [-time_step * multipliers[far_halo, j + 1, :, lanes] for j in range(steps - 1)]
        values.append(jnp.zeros_like(values[0]))
        for k, value in enumerate(pack(*real_transform(values))):
            packed[far_row, k, :, lanes] += value

    for block in range(blocks - 1):
        add_far(block)

    @pl.when(jnp.logical_not(hub))
    def _():
        gather_sums.wait_send()
        share_sums.wait_recv()

    misfit[...] = total[:steps] / total[steps : steps + 1] - wanted[...]
    add_far(blocks - 1)

    arrive(multipliers.at[far_halo, pl.ds(1, steps - 1)], far_send.at[1])

    @pl.when(hub)
    def _():
        arrive(held.at[far_halo, pl.ds(0, steps)], far_send.at[0])
        arrive(gathered, chain_sem.at[0])
        share_sums.wait_send()


def solve(count, state, adjoint, control, regions, target, mask):
    steps, rows, planes, width = control.shape
    count_regions = target.shape[1]
    padded = (steps + 8, count_regions)
    blocks = width // 128
    f32, dma, vmem = jnp.float32, pltpu.SemaphoreType.DMA, pltpu.VMEM
    in_vmem = pl.BlockSpec(memory_space=pltpu.VMEM)
    return pl.pallas_call(
        functools.partial(solve_kernel, count),
        out_shape=(
            vmem((2,) + control.shape, f32),
            vmem((rows, steps, planes, width), f32),
            vmem(control.shape, f32),
            vmem(target.shape, f32),
            vmem(regions.shape, jnp.int32),
        ),
        in_specs=[HBM] * 6,
        out_specs=(in_vmem,) * 5,
        scratch_shapes=[
            vmem((rows, planes, steps, width), f32),
            vmem((rows + 2, steps + 1, planes, width), f32),
            vmem((rows + 2, steps, planes, width), f32),
            vmem((rows, steps, planes, width), f32),
            vmem(target.shape, f32),
            pltpu.SMEM(mask.shape, jnp.int32),
            vmem((steps, planes, width), f32),
        ]
        + [vmem(padded, f32)] * 6
        + [
            vmem((count // 4 - 1,) + padded, f32),
            dma((7,)),
            pltpu.SemaphoreType.REGULAR,
            dma((2,)),
            dma((2,)),
            dma((2,)),
            dma((1 + blocks,)),
            dma((3,)),
            dma((3,)),
            dma((2,)),
        ],
        compiler_params=pltpu.CompilerParams(
            collective_id=0, has_side_effects=True, vmem_limit_bytes=24 * 2**20
        ),
        name="solve",
    )(state, adjoint, control, regions, target, mask)


def finish_kernel(
    state_buffer, packed, gradient, misfit, labels,
    state_out, adjoint_out, gradient_out,
    adjoint_buffer, table, out_sem,
):
    steps, rows, planes, width = gradient.shape
    writes = [
        pltpu.make_async_copy(state_buffer, state_out, out_sem.at[0]),
        pltpu.make_async_copy(gradient, gradient_out, out_sem.at[1]),
    ]
    for write in writes:
        write.start()

    values = real_transform([jnp.broadcast_to(misfit[j : j + 1], (8, table.shape[2])) for j in range(steps)])
    for k, value in enumerate(pack(*values)):
        table[k] = value

    def row_body(y, carry):
        for block in range(width // 128):
            lanes = pl.ds(block * 128, 128)
            ids = labels[y, :, lanes]
            values = [
                packed[y, k, :, lanes] + jnp.take_along_axis(table[k], ids, axis=1, mode="promise_in_bounds")
                for k in range(steps)
            ]
            top = steps // 2 + 1
            imag = [None] + values[top:] + [None] * (2 * top - 1 - steps)

            def put(part, k, value):
                adjoint_buffer[part, y, k, :, lanes] = value

            write_spectrum(put, values[:top], imag, steps)
        for part in range(2):
            pltpu.make_async_copy(
                adjoint_buffer.at[part, y], adjoint_out.at[part, pl.ds(0, steps), y], out_sem.at[2]
            ).start()
        return carry

    lax.fori_loop(0, rows, row_body, 0)
    for write in writes:
        write.wait()
    pltpu.make_async_copy(adjoint_buffer, adjoint_buffer, out_sem.at[2]).wait()


def finish(control, state_buffer, packed, gradient, misfit, labels):
    steps, rows, planes, width = control.shape
    f32, dma = jnp.float32, pltpu.SemaphoreType.DMA
    in_vmem = pl.BlockSpec(memory_space=pltpu.VMEM)
    spectrum_shape = jax.ShapeDtypeStruct((2,) + control.shape, f32)
    return pl.pallas_call(
        finish_kernel,
        out_shape=(spectrum_shape, spectrum_shape, jax.ShapeDtypeStruct(control.shape, f32)),
        in_specs=[in_vmem] * 5,
        out_specs=(HBM,) * 3,
        scratch_shapes=[
            pltpu.VMEM((2, rows, steps, planes, width), f32),
            pltpu.VMEM((steps, 8, misfit.shape[1]), f32),
            dma((3,)),
        ],
        compiler_params=pltpu.CompilerParams(vmem_limit_bytes=16 * 2**20),
        name="finish",
    )(state_buffer, packed, gradient, misfit, labels)


def on_device(count, *arrays):
    state, adjoint, control, target, mask, regions = (
        pltpu.with_memory_space_constraint(array, pltpu.HBM) for array in arrays
    )
    found = solve(count, state, adjoint, control, regions, target, mask)
    return finish(control, *found)


def solution(mesh):
    return jax.shard_map(
        functools.partial(on_device, mesh.shape["space"]),
        mesh=mesh,
        in_specs=(
            P("parts", "space", None, None),
            P("parts", "space", None, None),
            P("parts", "space", None, None),
            P("parts", None),
            P("space", "parts"),
            P("space", "parts", None),
        ),
        out_specs=(
            P(None, "parts", "space", None, None),
            P(None, "parts", "space", None, None),
            P("parts", "space", None, None),
        ),
        check_vma=False,
    )
```

```python
import functools
import math

import jax
import jax.numpy as jnp
from jax import lax
from jax.experimental import pallas as pl
from jax.experimental.pallas import tpu as pltpu
from jax.sharding import PartitionSpec as P

time_step = 0.15
penalty = 0.5
MESH = pl.DeviceIdType.MESH
HBM = pl.BlockSpec(memory_space=pltpu.HBM)
RELAY_STEPS = 4


def real_transform(values):
    n = len(values)
    if n == 1:
        return [values[0]], [None]
    if n % 2:
        real, imag = [], []
        for k in range(n // 2 + 1):
            angles = [2.0 * math.pi * (j * k % n) / n for j in range(n)]
            real.append(sum(v * math.cos(a) for v, a in zip(values, angles)))
            imag.append(None if k == 0 else sum(v * -math.sin(a) for v, a in zip(values, angles)))
        return real, imag
    even_re, even_im = real_transform(values[::2])
    odd_re, odd_im = real_transform(values[1::2])
    m = n // 2
    real, imag = [None] * (m + 1), [None] * (m + 1)
    for k in range(m // 2 + 1):
        a_re, a_im, b_re, b_im = even_re[k], even_im[k], odd_re[k], odd_im[k]
        if k == 0:
            real[0], real[m] = a_re + b_re, a_re - b_re
            continue
        if 2 * k == m:
            real[k], imag[k] = a_re, -b_re
            continue
        c, s = math.cos(2.0 * math.pi * k / n), math.sin(2.0 * math.pi * k / n)
        t_re, t_im = c * b_re + s * b_im, c * b_im - s * b_re
        real[k], imag[k] = a_re + t_re, a_im + t_im
        real[m - k], imag[m - k] = a_re - t_re, t_im - a_im
    return real, imag


def write_spectrum(put, real, imag, n):
    zero = jnp.zeros_like(real[0])
    for k in range(n):
        low = min(k, n - k)
        put(0, k, real[low])
        value = imag[low]
        put(1, k, zero if value is None else (value if k == low else -value))


def pack(real, imag):
    return real + [value for value in imag if value is not None]


def solve_kernel(
    count, state, adjoint, control, regions, target, mask,
    state_buffer, packed, gradient, misfit, labels,
    sampled, held, multipliers, heat, wanted, allowed, residual, partial, paired, joined, crossed, summed, total, gathered, parcel,
    load_sem, ready, near_send, near_recv, far_send, far_recv, sum_send, sum_recv, chain_sem, relay_sem,
):
    steps, rows, planes, width = control.shape
    count_regions = target.shape[1]
    blocks = width // 128
    links = count // 4
    me = lax.axis_index("space")
    link, place = me // 4, me % 4
    odd = me % 2
    partner = me + 1 - 2 * odd
    outside = (me + count - 1 + 2 * odd) % count
    hub = (place == 0) | (place == 3)
    last = me == count - 1
    origin = me == 0
    relays = min(links - 1, 3)
    carried = RELAY_STEPS
    direct = steps - 1 - relays * carried
    relay = (place == 0) & (link >= 1) & (link <= relays)
    helpers = [4 * (d + 1) for d in range(relays) if d + 1 < links - 1]
    mate = link * 4 + 3 - place
    peers = [((link + d) % links) * 4 + place for d in range(1, links)]
    near_row, far_row = (1 - odd) * (rows - 1), odd * (rows - 1)
    near_halo, far_halo = (1 - odd) * (rows + 1), odd * (rows + 1)

    barrier = pltpu.get_barrier_semaphore()

    def greet(other):
        pl.semaphore_signal(barrier, inc=1, device_id={"space": other}, device_id_type=MESH)

    greet(partner)
    greet(outside)

    @pl.when(hub)
    def _():
        for other in [mate] + peers:
            greet(other)

    @pl.when(relay & (link < links - 1))
    def _():
        greet(count - 1)

    label_load = pltpu.make_async_copy(regions, labels, load_sem.at[0])

    def local(source, into, sem):
        return pltpu.make_async_copy(source, into, sem)

    sample_loads = [
        local(state.at[pl.ds(1, steps), y, plane], sampled.at[y, plane], load_sem.at[1])
        for y in range(rows)
        for plane in range(planes)
    ]
    later_loads = [local(target, wanted, load_sem.at[2]), local(mask, allowed, load_sem.at[3])]
    own = pl.ds(1, rows)
    for y in range(rows):
        later_loads += [
            local(adjoint.at[pl.ds(0, steps), y], multipliers.at[y + 1], load_sem.at[4]),
            local(control.at[pl.ds(0, steps), y], heat.at[y], load_sem.at[5]),
            local(state.at[pl.ds(0, steps + 1), y], held.at[y + 1], load_sem.at[6]),
        ]
    def arrive(ref, sem):
        local(ref, ref, sem).wait()

    near_copies, far_copies = [], []
    for source, first, target_rows, shift, length in (
        (state, 0, held, 0, steps), (adjoint, 1, multipliers, 1, steps - 1),
    ):
        n = len(near_copies)
        near_copies.append(
            pltpu.make_async_remote_copy(
                src_ref=source.at[pl.ds(first, length), near_row],
                dst_ref=target_rows.at[odd * (rows + 1), pl.ds(shift, length)],
                send_sem=near_send.at[n],
                recv_sem=near_recv.at[n],
                device_id={"space": partner},
                device_id_type=MESH,
            )
        )
        for block in range(blocks):
            lanes = pl.ds(block * 128, 128)
            n = len(far_copies)
            far_copies.append(
                pltpu.make_async_remote_copy(
                    src_ref=source.at[pl.ds(first, length), far_row, :, lanes],
                    dst_ref=target_rows.at[(1 - odd) * (rows + 1), pl.ds(shift, length), :, lanes],
                    send_sem=far_send.at[n // blocks],
                    recv_sem=far_recv.at[max(n - blocks + 1, 0)],
                    device_id={"space": outside},
                    device_id_type=MESH,
                )
            )

    lanes = pl.ds((blocks - 1) * 128, 128)
    short_copy = pltpu.make_async_remote_copy(
        src_ref=adjoint.at[pl.ds(1, direct), far_row, :, lanes],
        dst_ref=multipliers.at[(1 - odd) * (rows + 1), pl.ds(1, direct), :, lanes],
        send_sem=far_send.at[1],
        recv_sem=far_recv.at[blocks],
        device_id={"space": outside},
        device_id_type=MESH,
    )
    relay_out = [
        pltpu.make_async_remote_copy(
            src_ref=adjoint.at[pl.ds(1 + direct + d * carried, carried), far_row, :, lanes],
            dst_ref=parcel,
            send_sem=far_send.at[1],
            recv_sem=relay_sem.at[0],
            device_id={"space": jnp.int32(4 * (d + 1))},
            device_id_type=MESH,
        )
        for d in range(relays)
    ]
    relay_on = pltpu.make_async_remote_copy(
        src_ref=parcel,
        dst_ref=multipliers.at[0, pl.ds(1 + direct + (link - 1) * carried, carried), :, lanes],
        send_sem=relay_sem.at[1],
        recv_sem=relay_sem.at[2],
        device_id={"space": jnp.int32(0)},
        device_id_type=MESH,
    )

    def message(n, source, into, other):
        return pltpu.make_async_remote_copy(
            src_ref=source, dst_ref=into, send_sem=sum_send.at[n], recv_sem=sum_recv.at[n],
            device_id={"space": other}, device_id_type=MESH,
        )

    gather_sums = message(0, partial, paired, partner)
    cross_sums = message(1, joined, crossed, mate)
    share_sums = message(2, total, total, partner)
    chain_sums = [
        pltpu.make_async_remote_copy(
            src_ref=summed, dst_ref=gathered.at[d], send_sem=chain_sem.at[0], recv_sem=chain_sem.at[1],
            device_id={"space": peer}, device_id_type=MESH,
        )
        for d, peer in enumerate(peers)
    ]

    region_ids = lax.broadcasted_iota(jnp.int32, (count_regions, width), 0).astype(jnp.float32).astype(jnp.bfloat16)
    yes = jnp.ones((count_regions, width), jnp.bfloat16)
    no = jnp.zeros((count_regions, width), jnp.bfloat16)

    def add_row(row, carry):
        values = jnp.concatenate([sampled[row, plane] for plane in range(planes)], axis=1)
        high = values.astype(jnp.bfloat16)
        low = (values - high.astype(jnp.float32)).astype(jnp.bfloat16)
        ones = jnp.ones((16, planes * width), jnp.bfloat16)
        stacked = jnp.concatenate([high, low, ones], axis=0)
        onehot = jnp.concatenate(
            [
                jnp.where(
                    labels[row, pl.ds(plane, 1), :].astype(jnp.float32).astype(jnp.bfloat16) == region_ids, yes, no
                )
                for plane in range(planes)
            ],
            axis=1,
        )
        return carry + lax.dot_general(
            stacked, onehot, (((1,), (1,)), ((), ())), preferred_element_type=jnp.float32
        )

    def meet():
        pl.semaphore_wait(barrier, 2)
        for copy in far_copies:
            copy.start()
        pl.semaphore_signal(ready, inc=1, device_id={"space": outside}, device_id_type=MESH)

    pl.when(place == 2)(meet)
    label_load.start()
    for load in sample_loads:
        load.start()
    pl.when(place == 1)(meet)

    label_load.wait()
    arrive(sampled, load_sem.at[1])
    found = jnp.zeros((2 * steps + 16, count_regions), jnp.float32)
    for y in range(rows):
        found = add_row(y, found)
    partial[:steps] = found[:steps] + found[steps : 2 * steps]
    partial[steps:] = found[2 * steps : 2 * steps + 8]

    @pl.when(jnp.logical_not(hub))
    def _():
        pl.semaphore_wait(ready, 1)
        gather_sums.start()
        for copy in near_copies:
            copy.start()
        arrive(held.at[far_halo, pl.ds(0, steps)], far_send.at[0])

    for load in later_loads:
        load.start()

    @pl.when(last)
    def _():
        pl.semaphore_wait(barrier, 3 + len(peers) + len(helpers))
        for copy in relay_out + far_copies[:-1] + [short_copy]:
            copy.start()

    @pl.when(hub)
    def _():
        gather_sums.wait_recv()
        joined[...] = partial[...] + paired[...]
        cross_sums.start()
        for copy in near_copies:
            copy.start()

        @pl.when(jnp.logical_not(last | origin))
        def _():
            pl.semaphore_wait(barrier, 3 + len(peers))

        @pl.when((place == 0) & jnp.logical_not(origin))
        def _():
            for copy in far_copies[:blocks]:
                copy.start()

    lane = lax.broadcasted_iota(jnp.int32, (planes, width), 1)
    plane_ids = lax.broadcasted_iota(jnp.int32, (planes, width), 0)
    first_lane, last_lane = lane == 0, lane == width - 1
    first_plane, last_plane = plane_ids == 0, plane_ids == planes - 1

    def support_of(y):
        support = jnp.zeros((planes, width), jnp.float32)
        for plane in range(planes):
            support = jnp.where(plane_ids == plane, allowed[y, plane].astype(jnp.float32), support)
        return support

    def laplace(values, beside):
        total = beside + jnp.where(first_lane, 0.0, pltpu.roll(values, 1, 1))
        total = total + jnp.where(last_lane, 0.0, pltpu.roll(values, width - 1, 1))
        total = total + jnp.where(first_plane, 0.0, pltpu.roll(values, 1, 0))
        total = total + jnp.where(last_plane, 0.0, pltpu.roll(values, planes - 1, 0))
        return total - 6.0 * values

    def adjoint_transform(y, beside):
        def step(j, carry):
            later = multipliers[y + 1, j + 1]
            residual[j] = multipliers[y + 1, j] - later - time_step * laplace(later, beside(j + 1))
            return carry

        lax.fori_loop(0, steps - 1, step, 0, unroll=True)
        residual[steps - 1] = multipliers[y + 1, steps - 1]
        for block in range(blocks):
            lanes = pl.ds(block * 128, 128)
            values = real_transform([residual[j, :, lanes] for j in range(steps)])
            for k, value in enumerate(pack(*values)):
                packed[y, k, :, lanes] = value

    def adjoint_full(y, carry):
        adjoint_transform(y, lambda j: multipliers[y, j] + multipliers[y + 2, j])
        return carry

    def state_row(y, carry):
        support = support_of(y)

        def step(j, inner):
            now = held[y + 1, j]
            lap = laplace(now, held[y, j] + held[y + 2, j])
            residual[j] = held[y + 1, j + 1] - now - time_step * lap - time_step * support * heat[y, j]
            return inner

        lax.fori_loop(0, steps, step, 0, unroll=True)
        for block in range(blocks):
            lanes = pl.ds(block * 128, 128)
            real, imag = real_transform([residual[j, :, lanes] for j in range(steps)])

            def put(part, k, value):
                state_buffer[part, k, y, :, lanes] = value

            write_spectrum(put, real, imag, steps)
        return carry

    def gradient_row(y, carry):
        support = support_of(y)

        def step(j, inner):
            gradient[j, y] = penalty * heat[y, j] - support * multipliers[y + 1, j]
            return inner

        return lax.fori_loop(0, steps, step, carry, unroll=True)

    for load in later_loads[:2]:
        load.wait()
    arrive(multipliers.at[own], load_sem.at[4])

    lax.fori_loop(1, rows - 1, adjoint_full, 0)

    adjoint_transform(far_row, lambda j: multipliers[far_row + 2 - 2 * odd, j])

    arrive(heat, load_sem.at[5])
    arrive(held.at[own], load_sem.at[6])

    lax.fori_loop(0, rows, gradient_row, 0)

    @pl.when(origin)
    def _():
        pl.semaphore_wait(barrier, 3 + len(peers))
        far_copies[0].start()

    @pl.when(hub)
    def _():
        cross_sums.wait()
        summed[...] = joined[...] + crossed[...]
        for send in chain_sums:
            send.start()

        @pl.when(relay)
        def _():
            arrive(parcel, relay_sem.at[0])
            relay_on.start()

        @pl.when(jnp.logical_not(last | origin))
        def _():
            @pl.when(place == 3)
            def _():
                for copy in far_copies[:blocks]:
                    copy.start()

            for copy in far_copies[blocks:]:
                copy.start()

    lax.fori_loop(1, rows - 1, state_row, 0)

    for copy in near_copies:
        copy.wait()
    lax.fori_loop(near_row, near_row + 1, adjoint_full, 0)
    lax.fori_loop(near_row, near_row + 1, state_row, 0)

    @pl.when(origin)
    def _():
        for copy in far_copies[1:]:
            copy.start()

    @pl.when(hub)
    def _():
        result = summed[...]
        arrive(gathered, chain_sem.at[1])
        for d in range(len(peers)):
            result = result + gathered[d]
        total[...] = result
        share_sums.start()

    arrive(held.at[far_halo, pl.ds(0, steps)], far_recv.at[0])
    lax.fori_loop(far_row, far_row + 1, state_row, 0)

    def add_far(block):
        lanes = pl.ds(block * 128, 128)
        if block < blocks - 1:
            far_copies[blocks + block].wait_recv()
        else:
            pl.when(jnp.logical_not(origin))(far_copies[-1].wait_recv)

            @pl.when(origin)
            def _():
                short_copy.wait_recv()
                arrive(multipliers.at[0, pl.ds(1 + direct, relays * carried), :, lanes], relay_sem.at[2])

        values = [-time_step * multipliers[far_halo, j + 1, :, lanes] for j in range(steps - 1)]
        values.append(jnp.zeros_like(values[0]))
        for k, value in enumerate(pack(*real_transform(values))):
            packed[far_row, k, :, lanes] += value

    for block in range(blocks - 1):
        add_far(block)

    @pl.when(jnp.logical_not(hub))
    def _():
        gather_sums.wait_send()
        share_sums.wait_recv()

    misfit[...] = total[:steps] / total[steps : steps + 1] - wanted[...]
    add_far(blocks - 1)

    arrive(multipliers.at[far_halo, pl.ds(1, steps - 1)], far_send.at[1])

    @pl.when(relay)
    def _():
        arrive(parcel, relay_sem.at[1])

    @pl.when(hub)
    def _():
        arrive(held.at[far_halo, pl.ds(0, steps)], far_send.at[0])
        arrive(gathered, chain_sem.at[0])
        share_sums.wait_send()


def solve(count, state, adjoint, control, regions, target, mask):
    steps, rows, planes, width = control.shape
    count_regions = target.shape[1]
    padded = (steps + 8, count_regions)
    blocks = width // 128
    f32, dma, vmem = jnp.float32, pltpu.SemaphoreType.DMA, pltpu.VMEM
    in_vmem = pl.BlockSpec(memory_space=pltpu.VMEM)
    return pl.pallas_call(
        functools.partial(solve_kernel, count),
        out_shape=(
            vmem((2,) + control.shape, f32),
            vmem((rows, steps, planes, width), f32),
            vmem(control.shape, f32),
            vmem(target.shape, f32),
            vmem(regions.shape, jnp.int32),
        ),
        in_specs=[HBM] * 6,
        out_specs=(in_vmem,) * 5,
        scratch_shapes=[
            vmem((rows, planes, steps, width), f32),
            vmem((rows + 2, steps + 1, planes, width), f32),
            vmem((rows + 2, steps, planes, width), f32),
            vmem((rows, steps, planes, width), f32),
            vmem(target.shape, f32),
            pltpu.SMEM(mask.shape, jnp.int32),
            vmem((steps, planes, width), f32),
        ]
        + [vmem(padded, f32)] * 6
        + [
            vmem((count // 4 - 1,) + padded, f32),
            vmem((RELAY_STEPS, planes, 128), f32),
            dma((7,)),
            pltpu.SemaphoreType.REGULAR,
            dma((2,)),
            dma((2,)),
            dma((2,)),
            dma((1 + blocks,)),
            dma((3,)),
            dma((3,)),
            dma((2,)),
            dma((3,)),
        ],
        compiler_params=pltpu.CompilerParams(
            collective_id=0, has_side_effects=True, vmem_limit_bytes=24 * 2**20
        ),
        name="solve",
    )(state, adjoint, control, regions, target, mask)


def finish_kernel(
    state_buffer, packed, gradient, misfit, labels,
    state_out, adjoint_out, gradient_out,
    adjoint_buffer, table, out_sem,
):
    steps, rows, planes, width = gradient.shape
    writes = [
        pltpu.make_async_copy(state_buffer, state_out, out_sem.at[0]),
        pltpu.make_async_copy(gradient, gradient_out, out_sem.at[1]),
    ]
    for write in writes:
        write.start()

    values = real_transform([jnp.broadcast_to(misfit[j : j + 1], (8, table.shape[2])) for j in range(steps)])
    for k, value in enumerate(pack(*values)):
        table[k] = value

    def row_body(y, carry):
        for block in range(width // 128):
            lanes = pl.ds(block * 128, 128)
            ids = labels[y, :, lanes]
            values = [
                packed[y, k, :, lanes] + jnp.take_along_axis(table[k], ids, axis=1, mode="promise_in_bounds")
                for k in range(steps)
            ]
            top = steps // 2 + 1
            imag = [None] + values[top:] + [None] * (2 * top - 1 - steps)

            def put(part, k, value):
                adjoint_buffer[part, y, k, :, lanes] = value

            write_spectrum(put, values[:top], imag, steps)
        for part in range(2):
            pltpu.make_async_copy(
                adjoint_buffer.at[part, y], adjoint_out.at[part, pl.ds(0, steps), y], out_sem.at[2]
            ).start()
        return carry

    lax.fori_loop(0, rows, row_body, 0)
    for write in writes:
        write.wait()
    pltpu.make_async_copy(adjoint_buffer, adjoint_buffer, out_sem.at[2]).wait()


def finish(control, state_buffer, packed, gradient, misfit, labels):
    steps, rows, planes, width = control.shape
    f32, dma = jnp.float32, pltpu.SemaphoreType.DMA
    in_vmem = pl.BlockSpec(memory_space=pltpu.VMEM)
    spectrum_shape = jax.ShapeDtypeStruct((2,) + control.shape, f32)
    return pl.pallas_call(
        finish_kernel,
        out_shape=(spectrum_shape, spectrum_shape, jax.ShapeDtypeStruct(control.shape, f32)),
        in_specs=[in_vmem] * 5,
        out_specs=(HBM,) * 3,
        scratch_shapes=[
            pltpu.VMEM((2, rows, steps, planes, width), f32),
            pltpu.VMEM((steps, 8, misfit.shape[1]), f32),
            dma((3,)),
        ],
        compiler_params=pltpu.CompilerParams(vmem_limit_bytes=16 * 2**20),
        name="finish",
    )(state_buffer, packed, gradient, misfit, labels)


def on_device(count, *arrays):
    state, adjoint, control, target, mask, regions = (
        pltpu.with_memory_space_constraint(array, pltpu.HBM) for array in arrays
    )
    found = solve(count, state, adjoint, control, regions, target, mask)
    return finish(control, *found)


def solution(mesh):
    return jax.shard_map(
        functools.partial(on_device, mesh.shape["space"]),
        mesh=mesh,
        in_specs=(
            P("parts", "space", None, None),
            P("parts", "space", None, None),
            P("parts", "space", None, None),
            P("parts", None),
            P("space", "parts"),
            P("space", "parts", None),
        ),
        out_specs=(
            P(None, "parts", "space", None, None),
            P(None, "parts", "space", None, None),
            P("parts", "space", None, None),
        ),
        check_vma=False,
    )
```

```python
import functools
import math

import jax
import jax.numpy as jnp
from jax import lax
from jax.experimental import pallas as pl
from jax.experimental.pallas import tpu as pltpu
from jax.sharding import PartitionSpec as P

time_step = 0.15
penalty = 0.5
MESH = pl.DeviceIdType.MESH
HBM = pl.BlockSpec(memory_space=pltpu.HBM)
RELAY_STEPS = 4


def real_transform(values):
    n = len(values)
    if n == 1:
        return [values[0]], [None]
    if n % 2:
        real, imag = [], []
        for k in range(n // 2 + 1):
            angles = [2.0 * math.pi * (j * k % n) / n for j in range(n)]
            real.append(sum(v * math.cos(a) for v, a in zip(values, angles)))
            imag.append(None if k == 0 else sum(v * -math.sin(a) for v, a in zip(values, angles)))
        return real, imag
    even_re, even_im = real_transform(values[::2])
    odd_re, odd_im = real_transform(values[1::2])
    m = n // 2
    real, imag = [None] * (m + 1), [None] * (m + 1)
    for k in range(m // 2 + 1):
        a_re, a_im, b_re, b_im = even_re[k], even_im[k], odd_re[k], odd_im[k]
        if k == 0:
            real[0], real[m] = a_re + b_re, a_re - b_re
            continue
        if 2 * k == m:
            real[k], imag[k] = a_re, -b_re
            continue
        c, s = math.cos(2.0 * math.pi * k / n), math.sin(2.0 * math.pi * k / n)
        t_re, t_im = c * b_re + s * b_im, c * b_im - s * b_re
        real[k], imag[k] = a_re + t_re, a_im + t_im
        real[m - k], imag[m - k] = a_re - t_re, t_im - a_im
    return real, imag


def write_spectrum(put, real, imag, n):
    zero = jnp.zeros_like(real[0])
    for k in range(n):
        low = min(k, n - k)
        put(0, k, real[low])
        value = imag[low]
        put(1, k, zero if value is None else (value if k == low else -value))


def pack(real, imag):
    return real + [value for value in imag if value is not None]


def halo_transform(multipliers, halo, lanes):
    steps = multipliers.shape[1]
    values = [-time_step * multipliers[halo, j + 1, :, lanes] for j in range(steps - 1)]
    values.append(jnp.zeros_like(values[0]))
    return pack(*real_transform(values))


def solve_kernel(
    count, state, adjoint, control, regions, target, mask,
    state_buffer, packed, gradient, misfit, labels, multipliers,
    sampled, held, heat, wanted, allowed, residual, partial, paired, joined, crossed, summed, total, gathered, parcel,
    load_sem, ready, near_send, near_recv, far_send, far_recv, sum_send, sum_recv, chain_sem, relay_sem,
):
    steps, rows, planes, width = control.shape
    count_regions = target.shape[1]
    blocks = width // 128
    links = count // 4
    me = lax.axis_index("space")
    link, place = me // 4, me % 4
    odd = me % 2
    partner = me + 1 - 2 * odd
    outside = (me + count - 1 + 2 * odd) % count
    hub = (place == 0) | (place == 3)
    last = me == count - 1
    origin = me == 0
    relays = min(links - 1, 3)
    carried = RELAY_STEPS
    direct = steps - 1 - relays * carried
    relay = (place == 0) & (link >= 1) & (link <= relays)
    helpers = [4 * (d + 1) for d in range(relays) if d + 1 < links - 1]
    mate = link * 4 + 3 - place
    peers = [((link + d) % links) * 4 + place for d in range(1, links)]
    near_row, far_row = (1 - odd) * (rows - 1), odd * (rows - 1)
    near_halo, far_halo = (1 - odd) * (rows + 1), odd * (rows + 1)

    barrier = pltpu.get_barrier_semaphore()

    def greet(other):
        pl.semaphore_signal(barrier, inc=1, device_id={"space": other}, device_id_type=MESH)

    greet(partner)
    greet(outside)

    @pl.when(hub)
    def _():
        for other in [mate] + peers:
            greet(other)

    @pl.when(relay & (link < links - 1))
    def _():
        greet(count - 1)

    label_load = pltpu.make_async_copy(regions, labels, load_sem.at[0])

    def local(source, into, sem):
        return pltpu.make_async_copy(source, into, sem)

    sample_loads = [
        local(state.at[pl.ds(1, steps), y, plane], sampled.at[y, plane], load_sem.at[1])
        for y in range(rows)
        for plane in range(planes)
    ]
    later_loads = [local(target, wanted, load_sem.at[2]), local(mask, allowed, load_sem.at[3])]
    own = pl.ds(1, rows)
    for y in range(rows):
        later_loads += [
            local(adjoint.at[pl.ds(0, steps), y], multipliers.at[y + 1], load_sem.at[4]),
            local(control.at[pl.ds(0, steps), y], heat.at[y], load_sem.at[5]),
            local(state.at[pl.ds(0, steps + 1), y], held.at[y + 1], load_sem.at[6]),
        ]
    def arrive(ref, sem):
        local(ref, ref, sem).wait()

    near_copies, far_copies = [], []
    for source, first, target_rows, shift, length in (
        (state, 0, held, 0, steps), (adjoint, 1, multipliers, 1, steps - 1),
    ):
        n = len(near_copies)
        near_copies.append(
            pltpu.make_async_remote_copy(
                src_ref=source.at[pl.ds(first, length), near_row],
                dst_ref=target_rows.at[odd * (rows + 1), pl.ds(shift, length)],
                send_sem=near_send.at[n],
                recv_sem=near_recv.at[n],
                device_id={"space": partner},
                device_id_type=MESH,
            )
        )
        for block in range(blocks):
            lanes = pl.ds(block * 128, 128)
            n = len(far_copies)
            far_copies.append(
                pltpu.make_async_remote_copy(
                    src_ref=source.at[pl.ds(first, length), far_row, :, lanes],
                    dst_ref=target_rows.at[(1 - odd) * (rows + 1), pl.ds(shift, length), :, lanes],
                    send_sem=far_send.at[n // blocks],
                    recv_sem=far_recv.at[max(n - blocks + 1, 0)],
                    device_id={"space": outside},
                    device_id_type=MESH,
                )
            )

    lanes = pl.ds((blocks - 1) * 128, 128)
    short_copy = pltpu.make_async_remote_copy(
        src_ref=adjoint.at[pl.ds(1, direct), far_row, :, lanes],
        dst_ref=multipliers.at[(1 - odd) * (rows + 1), pl.ds(1, direct), :, lanes],
        send_sem=far_send.at[1],
        recv_sem=far_recv.at[blocks],
        device_id={"space": outside},
        device_id_type=MESH,
    )
    relay_out = [
        pltpu.make_async_remote_copy(
            src_ref=adjoint.at[pl.ds(1 + direct + d * carried, carried), far_row, :, lanes],
            dst_ref=parcel,
            send_sem=far_send.at[1],
            recv_sem=relay_sem.at[0],
            device_id={"space": jnp.int32(4 * (d + 1))},
            device_id_type=MESH,
        )
        for d in range(relays)
    ]
    relay_on = pltpu.make_async_remote_copy(
        src_ref=parcel,
        dst_ref=multipliers.at[0, pl.ds(1 + direct + (link - 1) * carried, carried), :, lanes],
        send_sem=relay_sem.at[1],
        recv_sem=relay_sem.at[2],
        device_id={"space": jnp.int32(0)},
        device_id_type=MESH,
    )

    def message(n, source, into, other):
        source, into = source.at[pl.ds(0, steps + 1)], into.at[pl.ds(0, steps + 1)]
        return pltpu.make_async_remote_copy(
            src_ref=source, dst_ref=into, send_sem=sum_send.at[n], recv_sem=sum_recv.at[n],
            device_id={"space": other}, device_id_type=MESH,
        )

    gather_sums = message(0, partial, paired, partner)
    cross_sums = message(1, joined, crossed, mate)
    share_sums = message(2, total, total, partner)
    chain_sums = [
        pltpu.make_async_remote_copy(
            src_ref=summed.at[pl.ds(0, steps + 1)], dst_ref=gathered.at[d, pl.ds(0, steps + 1)], send_sem=chain_sem.at[0], recv_sem=chain_sem.at[1],
            device_id={"space": peer}, device_id_type=MESH,
        )
        for d, peer in enumerate(peers)
    ]

    region_ids = lax.broadcasted_iota(jnp.int32, (count_regions, width), 0).astype(jnp.float32).astype(jnp.bfloat16)
    yes = jnp.ones((count_regions, width), jnp.bfloat16)
    no = jnp.zeros((count_regions, width), jnp.bfloat16)

    def add_row(row, carry):
        values = jnp.concatenate([sampled[row, plane] for plane in range(planes)], axis=1)
        high = values.astype(jnp.bfloat16)
        low = (values - high.astype(jnp.float32)).astype(jnp.bfloat16)
        ones = jnp.ones((16, planes * width), jnp.bfloat16)
        stacked = jnp.concatenate([high, low, ones], axis=0)
        onehot = jnp.concatenate(
            [
                jnp.where(
                    labels[row, pl.ds(plane, 1), :].astype(jnp.float32).astype(jnp.bfloat16) == region_ids, yes, no
                )
                for plane in range(planes)
            ],
            axis=1,
        )
        return carry + lax.dot_general(
            stacked, onehot, (((1,), (1,)), ((), ())), preferred_element_type=jnp.float32
        )

    def meet():
        pl.semaphore_wait(barrier, 2)
        for copy in far_copies:
            copy.start()
        pl.semaphore_signal(ready, inc=1, device_id={"space": outside}, device_id_type=MESH)

    pl.when(place == 2)(meet)
    label_load.start()
    for load in sample_loads:
        load.start()
    pl.when(place == 1)(meet)

    label_load.wait()
    arrive(sampled, load_sem.at[1])
    found = jnp.zeros((2 * steps + 16, count_regions), jnp.float32)
    for y in range(rows):
        found = add_row(y, found)
    partial[:steps] = found[:steps] + found[steps : 2 * steps]
    partial[steps:] = found[2 * steps : 2 * steps + 8]

    @pl.when(jnp.logical_not(hub))
    def _():
        pl.semaphore_wait(ready, 1)
        gather_sums.start()
        for copy in near_copies:
            copy.start()
        arrive(held.at[far_halo, pl.ds(0, steps)], far_send.at[0])

    for load in later_loads:
        load.start()

    @pl.when(last)
    def _():
        pl.semaphore_wait(barrier, 3 + len(peers) + len(helpers))
        for copy in relay_out + far_copies[:-1] + [short_copy]:
            copy.start()

    @pl.when(hub)
    def _():
        gather_sums.wait_recv()
        joined[...] = partial[...] + paired[...]
        cross_sums.start()
        for copy in near_copies:
            copy.start()

        @pl.when(jnp.logical_not(last | origin))
        def _():
            pl.semaphore_wait(barrier, 3 + len(peers))

        @pl.when((place == 0) & jnp.logical_not(origin))
        def _():
            for copy in far_copies[:blocks]:
                copy.start()

    lane = lax.broadcasted_iota(jnp.int32, (planes, width), 1)
    plane_ids = lax.broadcasted_iota(jnp.int32, (planes, width), 0)
    first_lane, last_lane = lane == 0, lane == width - 1
    first_plane, last_plane = plane_ids == 0, plane_ids == planes - 1

    def support_of(y):
        support = jnp.zeros((planes, width), jnp.float32)
        for plane in range(planes):
            support = jnp.where(plane_ids == plane, allowed[y, plane].astype(jnp.float32), support)
        return support

    def laplace(values, beside):
        total = beside + jnp.where(first_lane, 0.0, pltpu.roll(values, 1, 1))
        total = total + jnp.where(last_lane, 0.0, pltpu.roll(values, width - 1, 1))
        total = total + jnp.where(first_plane, 0.0, pltpu.roll(values, 1, 0))
        total = total + jnp.where(last_plane, 0.0, pltpu.roll(values, planes - 1, 0))
        return total - 6.0 * values

    def adjoint_transform(y, beside):
        def step(j, carry):
            later = multipliers[y + 1, j + 1]
            residual[j] = multipliers[y + 1, j] - later - time_step * laplace(later, beside(j + 1))
            return carry

        lax.fori_loop(0, steps - 1, step, 0, unroll=True)
        residual[steps - 1] = multipliers[y + 1, steps - 1]
        for block in range(blocks):
            lanes = pl.ds(block * 128, 128)
            values = real_transform([residual[j, :, lanes] for j in range(steps)])
            for k, value in enumerate(pack(*values)):
                packed[y, k, :, lanes] = value

    def adjoint_full(y, carry):
        adjoint_transform(y, lambda j: multipliers[y, j] + multipliers[y + 2, j])
        return carry

    def state_row(y, carry):
        support = support_of(y)

        def step(j, inner):
            now = held[y + 1, j]
            lap = laplace(now, held[y, j] + held[y + 2, j])
            residual[j] = held[y + 1, j + 1] - now - time_step * lap - time_step * support * heat[y, j]
            return inner

        lax.fori_loop(0, steps, step, 0, unroll=True)
        for block in range(blocks):
            lanes = pl.ds(block * 128, 128)
            real, imag = real_transform([residual[j, :, lanes] for j in range(steps)])

            def put(part, k, value):
                state_buffer[part, k, y, :, lanes] = value

            write_spectrum(put, real, imag, steps)
        return carry

    def gradient_row(y, carry):
        support = support_of(y)

        def step(j, inner):
            gradient[j, y] = penalty * heat[y, j] - support * multipliers[y + 1, j]
            return inner

        return lax.fori_loop(0, steps, step, carry, unroll=True)

    for load in later_loads[:2]:
        load.wait()
    arrive(multipliers.at[own], load_sem.at[4])

    lax.fori_loop(1, rows - 1, adjoint_full, 0)

    adjoint_transform(far_row, lambda j: multipliers[far_row + 2 - 2 * odd, j])

    arrive(heat, load_sem.at[5])
    arrive(held.at[own], load_sem.at[6])

    lax.fori_loop(0, rows, gradient_row, 0)

    @pl.when(origin)
    def _():
        pl.semaphore_wait(barrier, 3 + len(peers))
        far_copies[0].start()

    @pl.when(hub)
    def _():
        cross_sums.wait()
        summed[...] = joined[...] + crossed[...]
        for send in chain_sums:
            send.start()

        @pl.when(relay)
        def _():
            arrive(parcel, relay_sem.at[0])
            relay_on.start()

        @pl.when(jnp.logical_not(last | origin))
        def _():
            @pl.when(place == 0)
            def _():
                for copy in far_copies[blocks:]:
                    copy.start()

    lax.fori_loop(1, rows - 1, state_row, 0)

    @pl.when((place == 3) & jnp.logical_not(last))
    def _():
        for copy in far_copies:
            copy.start()


    for copy in near_copies:
        copy.wait()
    lax.fori_loop(near_row, near_row + 1, adjoint_full, 0)
    lax.fori_loop(near_row, near_row + 1, state_row, 0)

    @pl.when(origin)
    def _():
        for copy in far_copies[1:]:
            copy.start()

    @pl.when(hub)
    def _():
        result = summed[...]
        arrive(gathered.at[:, pl.ds(0, steps + 1)], chain_sem.at[1])
        for d in range(len(peers)):
            result = result + gathered[d]
        total[...] = result
        share_sums.start()

    arrive(held.at[far_halo, pl.ds(0, steps)], far_recv.at[0])
    lax.fori_loop(far_row, far_row + 1, state_row, 0)

    def add_far(block):
        lanes = pl.ds(block * 128, 128)
        if block < blocks - 1:
            far_copies[blocks + block].wait_recv()
        else:
            pl.when(jnp.logical_not(origin))(far_copies[-1].wait_recv)

            @pl.when(origin)
            def _():
                short_copy.wait_recv()
                arrive(multipliers.at[0, pl.ds(1 + direct, relays * carried), :, lanes], relay_sem.at[2])

        if block < blocks - 1:
            for k, value in enumerate(halo_transform(multipliers, far_halo, lanes)):
                packed[far_row, k, :, lanes] += value

    for block in range(blocks - 1):
        add_far(block)

    @pl.when(jnp.logical_not(hub))
    def _():
        gather_sums.wait_send()
        share_sums.wait_recv()

    misfit[...] = total[:steps] / total[steps : steps + 1] - wanted[...]
    add_far(blocks - 1)

    arrive(multipliers.at[far_halo, pl.ds(1, steps - 1)], far_send.at[1])

    @pl.when(relay)
    def _():
        arrive(parcel, relay_sem.at[1])

    @pl.when(hub)
    def _():
        arrive(held.at[far_halo, pl.ds(0, steps)], far_send.at[0])
        arrive(gathered.at[:, pl.ds(0, steps + 1)], chain_sem.at[0])
        share_sums.wait_send()


def solve(count, state, adjoint, control, regions, target, mask):
    steps, rows, planes, width = control.shape
    count_regions = target.shape[1]
    padded = (steps + 8, count_regions)
    blocks = width // 128
    f32, dma, vmem = jnp.float32, pltpu.SemaphoreType.DMA, pltpu.VMEM
    in_vmem = pl.BlockSpec(memory_space=pltpu.VMEM)
    return pl.pallas_call(
        functools.partial(solve_kernel, count),
        out_shape=(
            vmem((2,) + control.shape, f32),
            vmem((rows, steps, planes, width), f32),
            vmem(control.shape, f32),
            vmem(target.shape, f32),
            vmem(regions.shape, jnp.int32),
            vmem((rows + 2, steps, planes, width), f32),
        ),
        in_specs=[HBM] * 6,
        out_specs=(in_vmem,) * 6,
        scratch_shapes=[
            vmem((rows, planes, steps, width), f32),
            vmem((rows + 2, steps + 1, planes, width), f32),
            vmem((rows, steps, planes, width), f32),
            vmem(target.shape, f32),
            pltpu.SMEM(mask.shape, jnp.int32),
            vmem((steps, planes, width), f32),
        ]
        + [vmem(padded, f32)] * 6
        + [
            vmem((count // 4 - 1,) + padded, f32),
            vmem((RELAY_STEPS, planes, 128), f32),
            dma((7,)),
            pltpu.SemaphoreType.REGULAR,
            dma((2,)),
            dma((2,)),
            dma((2,)),
            dma((1 + blocks,)),
            dma((3,)),
            dma((3,)),
            dma((2,)),
            dma((3,)),
        ],
        compiler_params=pltpu.CompilerParams(
            collective_id=0, has_side_effects=True, vmem_limit_bytes=24 * 2**20
        ),
        name="solve",
    )(state, adjoint, control, regions, target, mask)


def finish_kernel(
    state_buffer, packed, gradient, misfit, labels, multipliers,
    state_out, adjoint_out, gradient_out,
    adjoint_buffer, table, late, out_sem,
):
    steps, rows, planes, width = gradient.shape
    writes = [
        pltpu.make_async_copy(state_buffer, state_out, out_sem.at[0]),
        pltpu.make_async_copy(gradient, gradient_out, out_sem.at[1]),
    ]
    for write in writes:
        write.start()

    values = real_transform([jnp.broadcast_to(misfit[j : j + 1], (8, table.shape[2])) for j in range(steps)])
    for k, value in enumerate(pack(*values)):
        table[k] = value

    blocks = width // 128
    odd = lax.axis_index("space") % 2
    for k, value in enumerate(
        halo_transform(multipliers, odd * (rows + 1), pl.ds((blocks - 1) * 128, 128))
    ):
        late[0, k] = jnp.zeros_like(value)
        late[1, k] = value

    def row_body(y, carry):
        chosen = jnp.where(y == odd * (rows - 1), 1, 0)
        for block in range(blocks):
            lanes = pl.ds(block * 128, 128)
            ids = labels[y, :, lanes]
            values = [
                packed[y, k, :, lanes] + jnp.take_along_axis(table[k], ids, axis=1, mode="promise_in_bounds")
                for k in range(steps)
            ]
            if block == blocks - 1:
                values = [value + late[chosen, k] for k, value in enumerate(values)]
            top = steps // 2 + 1
            imag = [None] + values[top:] + [None] * (2 * top - 1 - steps)

            def put(part, k, value):
                adjoint_buffer[part, y, k, :, lanes] = value

            write_spectrum(put, values[:top], imag, steps)
        for part in range(2):
            pltpu.make_async_copy(
                adjoint_buffer.at[part, y], adjoint_out.at[part, pl.ds(0, steps), y], out_sem.at[2]
            ).start()
        return carry

    lax.fori_loop(0, rows, row_body, 0)
    for write in writes:
        write.wait()
    pltpu.make_async_copy(adjoint_buffer, adjoint_buffer, out_sem.at[2]).wait()


def finish(control, state_buffer, packed, gradient, misfit, labels, multipliers):
    steps, rows, planes, width = control.shape
    f32, dma = jnp.float32, pltpu.SemaphoreType.DMA
    in_vmem = pl.BlockSpec(memory_space=pltpu.VMEM)
    spectrum_shape = jax.ShapeDtypeStruct((2,) + control.shape, f32)
    return pl.pallas_call(
        finish_kernel,
        out_shape=(spectrum_shape, spectrum_shape, jax.ShapeDtypeStruct(control.shape, f32)),
        in_specs=[in_vmem] * 6,
        out_specs=(HBM,) * 3,
        scratch_shapes=[
            pltpu.VMEM((2, rows, steps, planes, width), f32),
            pltpu.VMEM((steps, 8, misfit.shape[1]), f32),
            pltpu.VMEM((2, steps, planes, 128), f32),
            dma((3,)),
        ],
        compiler_params=pltpu.CompilerParams(vmem_limit_bytes=16 * 2**20),
        name="finish",
    )(state_buffer, packed, gradient, misfit, labels, multipliers)


def on_device(count, *arrays):
    state, adjoint, control, target, mask, regions = (
        pltpu.with_memory_space_constraint(array, pltpu.HBM) for array in arrays
    )
    found = solve(count, state, adjoint, control, regions, target, mask)
    return finish(control, *found)


def solution(mesh):
    return jax.shard_map(
        functools.partial(on_device, mesh.shape["space"]),
        mesh=mesh,
        in_specs=(
            P("parts", "space", None, None),
            P("parts", "space", None, None),
            P("parts", "space", None, None),
            P("parts", None),
            P("space", "parts"),
            P("space", "parts", None),
        ),
        out_specs=(
            P(None, "parts", "space", None, None),
            P(None, "parts", "space", None, None),
            P("parts", "space", None, None),
        ),
        check_vma=False,
    )
```

```python
import functools
import math

import jax
import jax.numpy as jnp
from jax import lax
from jax.experimental import pallas as pl
from jax.experimental.pallas import tpu as pltpu
from jax.sharding import PartitionSpec as P

time_step = 0.15
penalty = 0.5
MESH = pl.DeviceIdType.MESH
HBM = pl.BlockSpec(memory_space=pltpu.HBM)
RELAY_STEPS = 4


def real_transform(values):
    n = len(values)
    if n == 1:
        return [values[0]], [None]
    if n % 2:
        real, imag = [], []
        for k in range(n // 2 + 1):
            angles = [2.0 * math.pi * (j * k % n) / n for j in range(n)]
            real.append(sum(v * math.cos(a) for v, a in zip(values, angles)))
            imag.append(None if k == 0 else sum(v * -math.sin(a) for v, a in zip(values, angles)))
        return real, imag
    even_re, even_im = real_transform(values[::2])
    odd_re, odd_im = real_transform(values[1::2])
    m = n // 2
    real, imag = [None] * (m + 1), [None] * (m + 1)
    for k in range(m // 2 + 1):
        a_re, a_im, b_re, b_im = even_re[k], even_im[k], odd_re[k], odd_im[k]
        if k == 0:
            real[0], real[m] = a_re + b_re, a_re - b_re
            continue
        if 2 * k == m:
            real[k], imag[k] = a_re, -b_re
            continue
        c, s = math.cos(2.0 * math.pi * k / n), math.sin(2.0 * math.pi * k / n)
        t_re, t_im = c * b_re + s * b_im, c * b_im - s * b_re
        real[k], imag[k] = a_re + t_re, a_im + t_im
        real[m - k], imag[m - k] = a_re - t_re, t_im - a_im
    return real, imag


def write_spectrum(put, real, imag, n):
    zero = jnp.zeros_like(real[0])
    for k in range(n):
        low = min(k, n - k)
        put(0, k, real[low])
        value = imag[low]
        put(1, k, zero if value is None else (value if k == low else -value))


def pack(real, imag):
    return real + [value for value in imag if value is not None]


def halo_transform(multipliers, halo, lanes):
    steps = multipliers.shape[1]
    values = [-time_step * multipliers[halo, j + 1, :, lanes] for j in range(steps - 1)]
    values.append(jnp.zeros_like(values[0]))
    return pack(*real_transform(values))


def solve_kernel(
    count, state, adjoint, control, regions, target, mask,
    state_buffer, packed, gradient, misfit, labels, multipliers,
    sampled, held, heat, wanted, allowed, residual, partial, paired, joined, crossed, summed, total, gathered, parcel,
    load_sem, ready, near_sem, far_send, far_recv, sum_sem, chain_sem, relay_sem,
):
    steps, rows, planes, width = control.shape
    count_regions = target.shape[1]
    blocks = width // 128
    links = count // 4
    me = lax.axis_index("space")
    link, place = me // 4, me % 4
    odd = me % 2
    partner = me + 1 - 2 * odd
    outside = (me + count - 1 + 2 * odd) % count
    hub = (place == 0) | (place == 3)
    last = me == count - 1
    origin = me == 0
    relays = min(links - 1, 3)
    carried = RELAY_STEPS
    direct = steps - 1 - relays * carried
    relay = (place == 0) & (link >= 1) & (link <= relays)
    helpers = [4 * (d + 1) for d in range(relays) if d + 1 < links - 1]
    mate = link * 4 + 3 - place
    peers = [((link + d) % links) * 4 + place for d in range(1, links)]
    near_row, far_row = (1 - odd) * (rows - 1), odd * (rows - 1)
    near_halo, far_halo = (1 - odd) * (rows + 1), odd * (rows + 1)

    barrier = pltpu.get_barrier_semaphore()

    def greet(other):
        pl.semaphore_signal(barrier, inc=1, device_id={"space": other}, device_id_type=MESH)

    greet(partner)
    greet(outside)

    @pl.when(hub)
    def _():
        for other in [mate] + peers:
            greet(other)

    @pl.when(relay & (link < links - 1))
    def _():
        greet(count - 1)

    label_load = pltpu.make_async_copy(regions, labels, load_sem.at[0])

    def local(source, into, sem):
        return pltpu.make_async_copy(source, into, sem)

    sample_loads = [
        local(state.at[pl.ds(1, steps), y, plane], sampled.at[y, plane], load_sem.at[0])
        for y in range(rows)
        for plane in range(planes)
    ]
    later_loads = [local(mask, allowed, load_sem.at[1]), local(target, wanted, load_sem.at[2])]
    own = pl.ds(1, rows)
    for y in range(rows):
        later_loads += [
            local(adjoint.at[pl.ds(0, steps), y], multipliers.at[y + 1], load_sem.at[3]),
            local(control.at[pl.ds(0, steps), y], heat.at[y], load_sem.at[4]),
            local(state.at[pl.ds(0, steps + 1), y], held.at[y + 1], load_sem.at[5]),
        ]
    def arrive(ref, sem):
        local(ref, ref, sem).wait()

    def arrive_slabs(count, sem):
        arrive(held.reshape((rows + 2) * (steps + 1), planes, width).at[pl.ds(0, count)], sem)

    near_copies, far_copies = [], []
    for source, first, target_rows, shift, length in (
        (state, 0, held, 0, steps), (adjoint, 1, multipliers, 1, steps - 1),
    ):
        n = len(near_copies)
        near_copies.append(
            pltpu.make_async_remote_copy(
                src_ref=source.at[pl.ds(first, length), near_row],
                dst_ref=target_rows.at[odd * (rows + 1), pl.ds(shift, length)],
                send_sem=near_sem.at[0],
                recv_sem=near_sem.at[1],
                device_id={"space": partner},
                device_id_type=MESH,
            )
        )
        for block in range(blocks):
            lanes = pl.ds(block * 128, 128)
            n = len(far_copies)
            far_copies.append(
                pltpu.make_async_remote_copy(
                    src_ref=source.at[pl.ds(first, length), far_row, :, lanes],
                    dst_ref=target_rows.at[(1 - odd) * (rows + 1), pl.ds(shift, length), :, lanes],
                    send_sem=far_send.at[n // blocks],
                    recv_sem=far_recv.at[max(n - blocks + 1, 0)],
                    device_id={"space": outside},
                    device_id_type=MESH,
                )
            )

    lanes = pl.ds((blocks - 1) * 128, 128)
    short_copy = pltpu.make_async_remote_copy(
        src_ref=adjoint.at[pl.ds(1, direct), far_row, :, lanes],
        dst_ref=multipliers.at[(1 - odd) * (rows + 1), pl.ds(1, direct), :, lanes],
        send_sem=far_send.at[1],
        recv_sem=far_recv.at[blocks],
        device_id={"space": outside},
        device_id_type=MESH,
    )
    relay_out = [
        pltpu.make_async_remote_copy(
            src_ref=adjoint.at[pl.ds(1 + direct + d * carried, carried), far_row, :, lanes],
            dst_ref=parcel,
            send_sem=far_send.at[1],
            recv_sem=relay_sem.at[0],
            device_id={"space": jnp.int32(4 * (d + 1))},
            device_id_type=MESH,
        )
        for d in range(relays)
    ]
    relay_on = pltpu.make_async_remote_copy(
        src_ref=parcel,
        dst_ref=multipliers.at[0, pl.ds(1 + direct + (link - 1) * carried, carried), :, lanes],
        send_sem=relay_sem.at[1],
        recv_sem=relay_sem.at[0],
        device_id={"space": jnp.int32(0)},
        device_id_type=MESH,
    )

    def message(n, source, into, other):
        source, into = source.at[pl.ds(0, steps + 1)], into.at[pl.ds(0, steps + 1)]
        return pltpu.make_async_remote_copy(
            src_ref=source, dst_ref=into, send_sem=sum_sem.at[0], recv_sem=sum_sem.at[1 + n % 2],
            device_id={"space": other}, device_id_type=MESH,
        )

    gather_sums = message(0, partial, paired, partner)
    cross_sums = message(1, joined, crossed, mate)
    share_sums = message(2, total, total, partner)
    chain_sums = [
        pltpu.make_async_remote_copy(
            src_ref=summed.at[pl.ds(0, steps + 1)], dst_ref=gathered.at[d, pl.ds(0, steps + 1)], send_sem=chain_sem.at[0], recv_sem=chain_sem.at[1],
            device_id={"space": peer}, device_id_type=MESH,
        )
        for d, peer in enumerate(peers)
    ]

    region_ids = lax.broadcasted_iota(jnp.int32, (count_regions, width), 0).astype(jnp.float32).astype(jnp.bfloat16)
    yes = jnp.ones((count_regions, width), jnp.bfloat16)
    no = jnp.zeros((count_regions, width), jnp.bfloat16)

    def add_row(row, carry):
        values = jnp.concatenate([sampled[row, plane] for plane in range(planes)], axis=1)
        high = values.astype(jnp.bfloat16)
        low = (values - high.astype(jnp.float32)).astype(jnp.bfloat16)
        ones = jnp.ones((16, planes * width), jnp.bfloat16)
        stacked = jnp.concatenate([high, low, ones], axis=0)
        onehot = jnp.concatenate(
            [
                jnp.where(
                    labels[row, pl.ds(plane, 1), :].astype(jnp.float32).astype(jnp.bfloat16) == region_ids, yes, no
                )
                for plane in range(planes)
            ],
            axis=1,
        )
        return carry + lax.dot_general(
            stacked, onehot, (((1,), (1,)), ((), ())), preferred_element_type=jnp.float32
        )

    def meet():
        pl.semaphore_wait(barrier, 2)
        for copy in far_copies:
            copy.start()
        pl.semaphore_signal(ready, inc=1, device_id={"space": outside}, device_id_type=MESH)

    pl.when(place == 2)(meet)
    label_load.start()
    for load in sample_loads:
        load.start()
    pl.when(place == 1)(meet)

    arrive_slabs(rows * (steps + 1), load_sem.at[0])
    found = jnp.zeros((2 * steps + 16, count_regions), jnp.float32)
    for y in range(rows):
        found = add_row(y, found)
    partial[:steps] = found[:steps] + found[steps : 2 * steps]
    partial[steps:] = found[2 * steps : 2 * steps + 8]

    @pl.when(jnp.logical_not(hub))
    def _():
        pl.semaphore_wait(ready, 1)
        gather_sums.start()
        for copy in near_copies:
            copy.start()
        arrive(held.at[far_halo, pl.ds(0, steps)], far_send.at[0])

    for load in later_loads:
        load.start()

    @pl.when(last)
    def _():
        pl.semaphore_wait(barrier, 3 + len(peers) + len(helpers))
        for copy in relay_out + far_copies[:-1] + [short_copy]:
            copy.start()

    @pl.when(hub)
    def _():
        gather_sums.wait_recv()
        joined[...] = partial[...] + paired[...]
        cross_sums.start()
        for copy in near_copies:
            copy.start()

        @pl.when(jnp.logical_not(last | origin))
        def _():
            pl.semaphore_wait(barrier, 3 + len(peers))

        @pl.when((place == 0) & jnp.logical_not(origin))
        def _():
            for copy in far_copies[:blocks]:
                copy.start()

    lane = lax.broadcasted_iota(jnp.int32, (planes, width), 1)
    plane_ids = lax.broadcasted_iota(jnp.int32, (planes, width), 0)
    first_lane, last_lane = lane == 0, lane == width - 1
    first_plane, last_plane = plane_ids == 0, plane_ids == planes - 1

    def support_of(y):
        support = jnp.zeros((planes, width), jnp.float32)
        for plane in range(planes):
            support = jnp.where(plane_ids == plane, allowed[y, plane].astype(jnp.float32), support)
        return support

    def laplace(values, beside):
        total = beside + jnp.where(first_lane, 0.0, pltpu.roll(values, 1, 1))
        total = total + jnp.where(last_lane, 0.0, pltpu.roll(values, width - 1, 1))
        total = total + jnp.where(first_plane, 0.0, pltpu.roll(values, 1, 0))
        total = total + jnp.where(last_plane, 0.0, pltpu.roll(values, planes - 1, 0))
        return total - 6.0 * values

    def adjoint_transform(y, beside):
        def step(j, carry):
            later = multipliers[y + 1, j + 1]
            residual[j] = multipliers[y + 1, j] - later - time_step * laplace(later, beside(j + 1))
            return carry

        lax.fori_loop(0, steps - 1, step, 0, unroll=True)
        residual[steps - 1] = multipliers[y + 1, steps - 1]
        for block in range(blocks):
            lanes = pl.ds(block * 128, 128)
            values = real_transform([residual[j, :, lanes] for j in range(steps)])
            for k, value in enumerate(pack(*values)):
                packed[y, k, :, lanes] = value

    def adjoint_full(y, carry):
        adjoint_transform(y, lambda j: multipliers[y, j] + multipliers[y + 2, j])
        return carry

    def state_row(y, carry):
        support = support_of(y)

        def step(j, inner):
            now = held[y + 1, j]
            lap = laplace(now, held[y, j] + held[y + 2, j])
            residual[j] = held[y + 1, j + 1] - now - time_step * lap - time_step * support * heat[y, j]
            return inner

        lax.fori_loop(0, steps, step, 0, unroll=True)
        for block in range(blocks):
            lanes = pl.ds(block * 128, 128)
            real, imag = real_transform([residual[j, :, lanes] for j in range(steps)])

            def put(part, k, value):
                state_buffer[part, k, y, :, lanes] = value

            write_spectrum(put, real, imag, steps)
        return carry

    def gradient_row(y, carry):
        support = support_of(y)

        def step(j, inner):
            gradient[j, y] = penalty * heat[y, j] - support * multipliers[y + 1, j]
            return inner

        return lax.fori_loop(0, steps, step, carry, unroll=True)

    for load in later_loads[:2]:
        load.wait()
    arrive(multipliers.at[own], load_sem.at[3])
    arrive(heat, load_sem.at[4])
    arrive(held.at[own], load_sem.at[5])

    lax.fori_loop(1, rows - 1, adjoint_full, 0)

    adjoint_transform(far_row, lambda j: multipliers[far_row + 2 - 2 * odd, j])

    lax.fori_loop(0, rows, gradient_row, 0)

    @pl.when(origin)
    def _():
        pl.semaphore_wait(barrier, 3 + len(peers))
        far_copies[0].start()

    @pl.when(hub)
    def _():
        cross_sums.wait()
        summed[...] = joined[...] + crossed[...]
        for send in chain_sums:
            send.start()

        @pl.when(relay)
        def _():
            arrive(parcel, relay_sem.at[0])
            relay_on.start()

        @pl.when(jnp.logical_not(last | origin))
        def _():
            @pl.when(place == 0)
            def _():
                for copy in far_copies[blocks:]:
                    copy.start()

    lax.fori_loop(1, rows - 1, state_row, 0)

    @pl.when((place == 3) & jnp.logical_not(last))
    def _():
        for copy in far_copies:
            copy.start()


    arrive_slabs(2 * steps - 1, near_sem.at[0])
    arrive_slabs(2 * steps - 1, near_sem.at[1])
    lax.fori_loop(near_row, near_row + 1, adjoint_full, 0)
    lax.fori_loop(near_row, near_row + 1, state_row, 0)

    @pl.when(origin)
    def _():
        for copy in far_copies[1:]:
            copy.start()

    @pl.when(hub)
    def _():
        result = summed[...]
        arrive(gathered.at[:, pl.ds(0, steps + 1)], chain_sem.at[1])
        for d in range(len(peers)):
            result = result + gathered[d]
        total[...] = result
        share_sums.start()

    arrive(held.at[far_halo, pl.ds(0, steps)], far_recv.at[0])
    lax.fori_loop(far_row, far_row + 1, state_row, 0)

    def add_far(block):
        lanes = pl.ds(block * 128, 128)
        if block < blocks - 1:
            far_copies[blocks + block].wait_recv()
        else:
            pl.when(jnp.logical_not(origin))(far_copies[-1].wait_recv)

            @pl.when(origin)
            def _():
                short_copy.wait_recv()
                arrive(multipliers.at[0, pl.ds(1 + direct, relays * carried), :, lanes], relay_sem.at[0])

        if block < blocks - 1:
            for k, value in enumerate(halo_transform(multipliers, far_halo, lanes)):
                packed[far_row, k, :, lanes] += value

    for block in range(blocks - 1):
        add_far(block)

    @pl.when(jnp.logical_not(hub))
    def _():
        gather_sums.wait_send()
        share_sums.wait_recv()

    misfit[...] = total[:steps] / total[steps : steps + 1] - wanted[...]
    add_far(blocks - 1)

    arrive(multipliers.at[far_halo, pl.ds(1, steps - 1)], far_send.at[1])

    @pl.when(relay)
    def _():
        arrive(parcel, relay_sem.at[1])

    @pl.when(hub)
    def _():
        arrive(held.at[far_halo, pl.ds(0, steps)], far_send.at[0])
        arrive(gathered.at[:, pl.ds(0, steps + 1)], chain_sem.at[0])
        share_sums.wait_send()


def solve(count, state, adjoint, control, regions, target, mask):
    steps, rows, planes, width = control.shape
    count_regions = target.shape[1]
    padded = (steps + 8, count_regions)
    blocks = width // 128
    f32, dma, vmem = jnp.float32, pltpu.SemaphoreType.DMA, pltpu.VMEM
    in_vmem = pl.BlockSpec(memory_space=pltpu.VMEM)
    return pl.pallas_call(
        functools.partial(solve_kernel, count),
        out_shape=(
            vmem((2,) + control.shape, f32),
            vmem((rows, steps, planes, width), f32),
            vmem(control.shape, f32),
            vmem(target.shape, f32),
            vmem(regions.shape, jnp.int32),
            vmem((rows + 2, steps, planes, width), f32),
        ),
        in_specs=[HBM] * 6,
        out_specs=(in_vmem,) * 6,
        scratch_shapes=[
            vmem((rows, planes, steps, width), f32),
            vmem((rows + 2, steps + 1, planes, width), f32),
            vmem((rows, steps, planes, width), f32),
            vmem(target.shape, f32),
            pltpu.SMEM(mask.shape, jnp.int32),
            vmem((steps, planes, width), f32),
        ]
        + [vmem(padded, f32)] * 6
        + [
            vmem((count // 4 - 1,) + padded, f32),
            vmem((RELAY_STEPS, planes, 128), f32),
            dma((6,)),
            pltpu.SemaphoreType.REGULAR,
            dma((2,)),
            dma((2,)),
            dma((1 + blocks,)),
            dma((3,)),
            dma((2,)),
            dma((2,)),
        ],
        compiler_params=pltpu.CompilerParams(
            collective_id=0, has_side_effects=True, vmem_limit_bytes=24 * 2**20
        ),
        name="solve",
    )(state, adjoint, control, regions, target, mask)


def finish_kernel(
    state_buffer, packed, gradient, misfit, labels, multipliers,
    state_out, adjoint_out, gradient_out,
    adjoint_buffer, table, late, out_sem,
):
    steps, rows, planes, width = gradient.shape
    writes = [
        pltpu.make_async_copy(state_buffer, state_out, out_sem.at[0]),
        pltpu.make_async_copy(gradient, gradient_out, out_sem.at[1]),
    ]
    for write in writes:
        write.start()

    values = real_transform([jnp.broadcast_to(misfit[j : j + 1], (8, table.shape[2])) for j in range(steps)])
    for k, value in enumerate(pack(*values)):
        table[k] = value

    blocks = width // 128
    odd = lax.axis_index("space") % 2
    for k, value in enumerate(
        halo_transform(multipliers, odd * (rows + 1), pl.ds((blocks - 1) * 128, 128))
    ):
        late[0, k] = jnp.zeros_like(value)
        late[1, k] = value

    def row_body(y, carry):
        chosen = jnp.where(y == odd * (rows - 1), 1, 0)
        for block in range(blocks):
            lanes = pl.ds(block * 128, 128)
            ids = labels[y, :, lanes]
            values = [
                packed[y, k, :, lanes] + jnp.take_along_axis(table[k], ids, axis=1, mode="promise_in_bounds")
                for k in range(steps)
            ]
            if block == blocks - 1:
                values = [value + late[chosen, k] for k, value in enumerate(values)]
            top = steps // 2 + 1
            imag = [None] + values[top:] + [None] * (2 * top - 1 - steps)

            def put(part, k, value):
                adjoint_buffer[part, y, k, :, lanes] = value

            write_spectrum(put, values[:top], imag, steps)
        for part in range(2):
            pltpu.make_async_copy(
                adjoint_buffer.at[part, y], adjoint_out.at[part, pl.ds(0, steps), y], out_sem.at[2]
            ).start()
        return carry

    lax.fori_loop(0, rows, row_body, 0)
    for write in writes:
        write.wait()
    pltpu.make_async_copy(adjoint_buffer, adjoint_buffer, out_sem.at[2]).wait()


def finish(control, state_buffer, packed, gradient, misfit, labels, multipliers):
    steps, rows, planes, width = control.shape
    f32, dma = jnp.float32, pltpu.SemaphoreType.DMA
    in_vmem = pl.BlockSpec(memory_space=pltpu.VMEM)
    spectrum_shape = jax.ShapeDtypeStruct((2,) + control.shape, f32)
    return pl.pallas_call(
        finish_kernel,
        out_shape=(spectrum_shape, spectrum_shape, jax.ShapeDtypeStruct(control.shape, f32)),
        in_specs=[in_vmem] * 6,
        out_specs=(HBM,) * 3,
        scratch_shapes=[
            pltpu.VMEM((2, rows, steps, planes, width), f32),
            pltpu.VMEM((steps, 8, misfit.shape[1]), f32),
            pltpu.VMEM((2, steps, planes, 128), f32),
            dma((3,)),
        ],
        compiler_params=pltpu.CompilerParams(vmem_limit_bytes=16 * 2**20),
        name="finish",
    )(state_buffer, packed, gradient, misfit, labels, multipliers)


def on_device(count, *arrays):
    state, adjoint, control, target, mask, regions = (
        pltpu.with_memory_space_constraint(array, pltpu.HBM) for array in arrays
    )
    found = solve(count, state, adjoint, control, regions, target, mask)
    return finish(control, *found)


def solution(mesh):
    return jax.shard_map(
        functools.partial(on_device, mesh.shape["space"]),
        mesh=mesh,
        in_specs=(
            P("parts", "space", None, None),
            P("parts", "space", None, None),
            P("parts", "space", None, None),
            P("parts", None),
            P("space", "parts"),
            P("space", "parts", None),
        ),
        out_specs=(
            P(None, "parts", "space", None, None),
            P(None, "parts", "space", None, None),
            P("parts", "space", None, None),
        ),
        check_vma=False,
    )
```

```python
import functools
import math

import jax
import jax.numpy as jnp
from jax import lax
from jax.experimental import pallas as pl
from jax.experimental.pallas import tpu as pltpu
from jax.sharding import PartitionSpec as P

time_step = 0.15
penalty = 0.5
MESH = pl.DeviceIdType.MESH
HBM = pl.BlockSpec(memory_space=pltpu.HBM)
RELAY_STEPS = 5


def real_transform(values):
    n = len(values)
    if n == 1:
        return [values[0]], [None]
    if n % 2:
        real, imag = [], []
        for k in range(n // 2 + 1):
            angles = [2.0 * math.pi * (j * k % n) / n for j in range(n)]
            real.append(sum(v * math.cos(a) for v, a in zip(values, angles)))
            imag.append(None if k == 0 else sum(v * -math.sin(a) for v, a in zip(values, angles)))
        return real, imag
    even_re, even_im = real_transform(values[::2])
    odd_re, odd_im = real_transform(values[1::2])
    m = n // 2
    real, imag = [None] * (m + 1), [None] * (m + 1)
    for k in range(m // 2 + 1):
        a_re, a_im, b_re, b_im = even_re[k], even_im[k], odd_re[k], odd_im[k]
        if k == 0:
            real[0], real[m] = a_re + b_re, a_re - b_re
            continue
        if 2 * k == m:
            real[k], imag[k] = a_re, -b_re
            continue
        c, s = math.cos(2.0 * math.pi * k / n), math.sin(2.0 * math.pi * k / n)
        t_re, t_im = c * b_re + s * b_im, c * b_im - s * b_re
        real[k], imag[k] = a_re + t_re, a_im + t_im
        real[m - k], imag[m - k] = a_re - t_re, t_im - a_im
    return real, imag


def write_spectrum(put, real, imag, n):
    zero = jnp.zeros_like(real[0])
    for k in range(n):
        low = min(k, n - k)
        put(0, k, real[low])
        value = imag[low]
        put(1, k, zero if value is None else (value if k == low else -value))


def pack(real, imag):
    return real + [value for value in imag if value is not None]


def halo_transform(multipliers, halo, lanes):
    steps = multipliers.shape[1]
    values = [-time_step * multipliers[halo, j + 1, :, lanes] for j in range(steps - 1)]
    values.append(jnp.zeros_like(values[0]))
    return pack(*real_transform(values))


def solve_kernel(
    count, state, adjoint, control, regions, target, mask,
    state_buffer, packed, gradient, misfit, labels, multipliers,
    sampled, held, heat, wanted, allowed, residual, partial, paired, joined, crossed, summed, total, gathered, parcel,
    load_sem, ready, near_sem, far_send, far_recv, sum_sem, chain_sem, relay_sem,
):
    steps, rows, planes, width = control.shape
    count_regions = target.shape[1]
    blocks = width // 128
    links = count // 4
    me = lax.axis_index("space")
    link, place = me // 4, me % 4
    odd = me % 2
    partner = me + 1 - 2 * odd
    outside = (me + count - 1 + 2 * odd) % count
    hub = (place == 0) | (place == 3)
    last = me == count - 1
    origin = me == 0
    relays = min(links - 1, 3)
    carried = RELAY_STEPS
    direct = steps - 1 - relays * carried
    relay = (place == 0) & (link >= 1) & (link <= relays)
    helpers = [4 * (d + 1) for d in range(relays) if d + 1 < links - 1]
    mate = link * 4 + 3 - place
    peers = [((link + d) % links) * 4 + place for d in range(1, links)]
    near_row, far_row = (1 - odd) * (rows - 1), odd * (rows - 1)
    near_halo, far_halo = (1 - odd) * (rows + 1), odd * (rows + 1)

    barrier = pltpu.get_barrier_semaphore()

    def greet(other):
        pl.semaphore_signal(barrier, inc=1, device_id={"space": other}, device_id_type=MESH)

    greet(partner)
    greet(outside)

    @pl.when(hub)
    def _():
        for other in [mate] + peers:
            greet(other)

    @pl.when(relay & (link < links - 1))
    def _():
        greet(count - 1)

    label_load = pltpu.make_async_copy(regions, labels, load_sem.at[0])

    def local(source, into, sem):
        return pltpu.make_async_copy(source, into, sem)

    sample_loads = [
        local(state.at[pl.ds(1, steps), y, plane], sampled.at[y, plane], load_sem.at[0])
        for y in range(rows)
        for plane in range(planes)
    ]
    later_loads = [local(mask, allowed, load_sem.at[1]), local(target, wanted, load_sem.at[2])]
    own = pl.ds(1, rows)
    for y in range(rows):
        later_loads += [
            local(adjoint.at[pl.ds(0, steps), y], multipliers.at[y + 1], load_sem.at[3]),
            local(control.at[pl.ds(0, steps), y], heat.at[y], load_sem.at[4]),
            local(state.at[pl.ds(0, steps + 1), y], held.at[y + 1], load_sem.at[5]),
        ]
    def arrive(ref, sem):
        local(ref, ref, sem).wait()

    def arrive_slabs(count, sem):
        arrive(held.reshape((rows + 2) * (steps + 1), planes, width).at[pl.ds(0, count)], sem)

    near_copies, far_copies = [], []
    for source, first, target_rows, shift, length in (
        (state, 0, held, 0, steps), (adjoint, 1, multipliers, 1, steps - 1),
    ):
        n = len(near_copies)
        near_copies.append(
            pltpu.make_async_remote_copy(
                src_ref=source.at[pl.ds(first, length), near_row],
                dst_ref=target_rows.at[odd * (rows + 1), pl.ds(shift, length)],
                send_sem=near_sem.at[0],
                recv_sem=near_sem.at[1],
                device_id={"space": partner},
                device_id_type=MESH,
            )
        )
        for block in range(blocks):
            lanes = pl.ds(block * 128, 128)
            n = len(far_copies)
            far_copies.append(
                pltpu.make_async_remote_copy(
                    src_ref=source.at[pl.ds(first, length), far_row, :, lanes],
                    dst_ref=target_rows.at[(1 - odd) * (rows + 1), pl.ds(shift, length), :, lanes],
                    send_sem=far_send.at[n // blocks],
                    recv_sem=far_recv.at[max(n - blocks + 1, 0)],
                    device_id={"space": outside},
                    device_id_type=MESH,
                )
            )

    lanes = pl.ds((blocks - 1) * 128, 128)
    short_copy = pltpu.make_async_remote_copy(
        src_ref=adjoint.at[pl.ds(1, direct), far_row, :, lanes],
        dst_ref=multipliers.at[(1 - odd) * (rows + 1), pl.ds(1, direct), :, lanes],
        send_sem=far_send.at[1],
        recv_sem=far_recv.at[blocks],
        device_id={"space": outside},
        device_id_type=MESH,
    )
    relay_out = [
        pltpu.make_async_remote_copy(
            src_ref=adjoint.at[pl.ds(1 + direct + d * carried, carried), far_row, :, lanes],
            dst_ref=parcel,
            send_sem=far_send.at[1],
            recv_sem=relay_sem.at[0],
            device_id={"space": jnp.int32(4 * (d + 1))},
            device_id_type=MESH,
        )
        for d in range(relays)
    ]
    relay_on = pltpu.make_async_remote_copy(
        src_ref=parcel,
        dst_ref=multipliers.at[0, pl.ds(1 + direct + (link + relays - 1) % relays * carried, carried), :, lanes],
        send_sem=relay_sem.at[1],
        recv_sem=relay_sem.at[0],
        device_id={"space": jnp.int32(0)},
        device_id_type=MESH,
    )

    def message(n, source, into, other):
        source, into = source.at[pl.ds(0, steps + 1)], into.at[pl.ds(0, steps + 1)]
        return pltpu.make_async_remote_copy(
            src_ref=source, dst_ref=into, send_sem=sum_sem.at[0], recv_sem=sum_sem.at[1 + n % 2],
            device_id={"space": other}, device_id_type=MESH,
        )

    gather_sums = message(0, partial, paired, partner)
    cross_sums = message(1, joined, crossed, mate)
    share_sums = message(2, total, total, partner)
    chain_sums = [
        pltpu.make_async_remote_copy(
            src_ref=summed.at[pl.ds(0, steps + 1)], dst_ref=gathered.at[d, pl.ds(0, steps + 1)], send_sem=chain_sem.at[0], recv_sem=chain_sem.at[1],
            device_id={"space": peer}, device_id_type=MESH,
        )
        for d, peer in enumerate(peers)
    ]

    region_ids = lax.broadcasted_iota(jnp.int32, (count_regions, width), 0).astype(jnp.float32).astype(jnp.bfloat16)
    yes = jnp.ones((count_regions, width), jnp.bfloat16)
    no = jnp.zeros((count_regions, width), jnp.bfloat16)

    def add_row(row, carry):
        values = jnp.concatenate([sampled[row, plane] for plane in range(planes)], axis=1)
        high = values.astype(jnp.bfloat16)
        low = (values - high.astype(jnp.float32)).astype(jnp.bfloat16)
        ones = jnp.ones((16, planes * width), jnp.bfloat16)
        stacked = jnp.concatenate([high, low, ones], axis=0)
        onehot = jnp.concatenate(
            [
                jnp.where(
                    labels[row, pl.ds(plane, 1), :].astype(jnp.float32).astype(jnp.bfloat16) == region_ids, yes, no
                )
                for plane in range(planes)
            ],
            axis=1,
        )
        return carry + lax.dot_general(
            stacked, onehot, (((1,), (1,)), ((), ())), preferred_element_type=jnp.float32
        )

    def meet():
        pl.semaphore_wait(barrier, 2)
        for copy in far_copies:
            copy.start()
        pl.semaphore_signal(ready, inc=1, device_id={"space": outside}, device_id_type=MESH)

    pl.when(place == 2)(meet)
    label_load.start()
    for load in sample_loads:
        load.start()
    pl.when(place == 1)(meet)

    arrive_slabs(rows * (steps + 1), load_sem.at[0])
    found = jnp.zeros((2 * steps + 16, count_regions), jnp.float32)
    for y in range(rows):
        found = add_row(y, found)
    partial[:steps] = found[:steps] + found[steps : 2 * steps]
    partial[steps:] = found[2 * steps : 2 * steps + 8]

    @pl.when(jnp.logical_not(hub))
    def _():
        pl.semaphore_wait(ready, 1)
        gather_sums.start()
        for copy in near_copies:
            copy.start()
        arrive(held.at[far_halo, pl.ds(0, steps)], far_send.at[0])

    for load in later_loads:
        load.start()

    @pl.when(last)
    def _():
        pl.semaphore_wait(barrier, 3 + len(peers) + len(helpers))
        for copy in relay_out + far_copies[:-1] + [short_copy]:
            copy.start()

    @pl.when(hub)
    def _():
        gather_sums.wait_recv()
        joined[...] = partial[...] + paired[...]
        cross_sums.start()
        for copy in near_copies:
            copy.start()

        @pl.when(jnp.logical_not(last | origin))
        def _():
            pl.semaphore_wait(barrier, 3 + len(peers))

        @pl.when((place == 0) & jnp.logical_not(origin))
        def _():
            for copy in far_copies[:blocks]:
                copy.start()

    lane = lax.broadcasted_iota(jnp.int32, (planes, width), 1)
    plane_ids = lax.broadcasted_iota(jnp.int32, (planes, width), 0)
    first_lane, last_lane = lane == 0, lane == width - 1
    first_plane, last_plane = plane_ids == 0, plane_ids == planes - 1

    def support_of(y):
        support = jnp.zeros((planes, width), jnp.float32)
        for plane in range(planes):
            support = jnp.where(plane_ids == plane, allowed[y, plane].astype(jnp.float32), support)
        return support

    def laplace(values, beside):
        total = beside + jnp.where(first_lane, 0.0, pltpu.roll(values, 1, 1))
        total = total + jnp.where(last_lane, 0.0, pltpu.roll(values, width - 1, 1))
        total = total + jnp.where(first_plane, 0.0, pltpu.roll(values, 1, 0))
        total = total + jnp.where(last_plane, 0.0, pltpu.roll(values, planes - 1, 0))
        return total - 6.0 * values

    def adjoint_transform(y, beside):
        def step(j, carry):
            later = multipliers[y + 1, j + 1]
            residual[j] = multipliers[y + 1, j] - later - time_step * laplace(later, beside(j + 1))
            return carry

        lax.fori_loop(0, steps - 1, step, 0, unroll=True)
        residual[steps - 1] = multipliers[y + 1, steps - 1]
        for block in range(blocks):
            lanes = pl.ds(block * 128, 128)
            values = real_transform([residual[j, :, lanes] for j in range(steps)])
            for k, value in enumerate(pack(*values)):
                packed[y, k, :, lanes] = value

    def adjoint_full(y, carry):
        adjoint_transform(y, lambda j: multipliers[y, j] + multipliers[y + 2, j])
        return carry

    def state_row(y, carry):
        support = support_of(y)

        def step(j, inner):
            now = held[y + 1, j]
            lap = laplace(now, held[y, j] + held[y + 2, j])
            residual[j] = held[y + 1, j + 1] - now - time_step * lap - time_step * support * heat[y, j]
            return inner

        lax.fori_loop(0, steps, step, 0, unroll=True)
        for block in range(blocks):
            lanes = pl.ds(block * 128, 128)
            real, imag = real_transform([residual[j, :, lanes] for j in range(steps)])

            def put(part, k, value):
                state_buffer[part, k, y, :, lanes] = value

            write_spectrum(put, real, imag, steps)
        return carry

    def gradient_row(y, carry):
        support = support_of(y)

        def step(j, inner):
            gradient[j, y] = penalty * heat[y, j] - support * multipliers[y + 1, j]
            return inner

        return lax.fori_loop(0, steps, step, carry, unroll=True)

    for load in later_loads[:2]:
        load.wait()
    arrive(multipliers.at[own], load_sem.at[3])
    arrive(heat, load_sem.at[4])
    arrive(held.at[own], load_sem.at[5])

    lax.fori_loop(1, rows - 1, adjoint_full, 0)

    adjoint_transform(far_row, lambda j: multipliers[far_row + 2 - 2 * odd, j])

    lax.fori_loop(0, rows, gradient_row, 0)

    @pl.when(origin)
    def _():
        pl.semaphore_wait(barrier, 3 + len(peers))
        far_copies[0].start()

    @pl.when(hub)
    def _():
        cross_sums.wait()
        summed[...] = joined[...] + crossed[...]
        for send in chain_sums:
            send.start()

        @pl.when(relay)
        def _():
            arrive(parcel, relay_sem.at[0])
            relay_on.start()

        @pl.when(jnp.logical_not(last | origin))
        def _():
            @pl.when(place == 0)
            def _():
                for copy in far_copies[blocks:]:
                    copy.start()

    lax.fori_loop(1, rows - 1, state_row, 0)

    @pl.when((place == 3) & jnp.logical_not(last))
    def _():
        for copy in far_copies:
            copy.start()


    arrive_slabs(2 * steps - 1, near_sem.at[0])
    arrive_slabs(2 * steps - 1, near_sem.at[1])
    lax.fori_loop(near_row, near_row + 1, adjoint_full, 0)
    lax.fori_loop(near_row, near_row + 1, state_row, 0)

    @pl.when(origin)
    def _():
        for copy in far_copies[1:]:
            copy.start()

    @pl.when(hub)
    def _():
        result = summed[...]
        arrive(gathered.at[:, pl.ds(0, steps + 1)], chain_sem.at[1])
        for d in range(len(peers)):
            result = result + gathered[d]
        total[...] = result
        share_sums.start()

    arrive(held.at[far_halo, pl.ds(0, steps)], far_recv.at[0])
    lax.fori_loop(far_row, far_row + 1, state_row, 0)

    def add_far(block):
        lanes = pl.ds(block * 128, 128)
        if block < blocks - 1:
            far_copies[blocks + block].wait_recv()
        else:
            pl.when(jnp.logical_not(origin))(far_copies[-1].wait_recv)

            @pl.when(origin)
            def _():
                short_copy.wait_recv()
                arrive(multipliers.at[0, pl.ds(1 + direct, relays * carried), :, lanes], relay_sem.at[0])

        if block < blocks - 1:
            for k, value in enumerate(halo_transform(multipliers, far_halo, lanes)):
                packed[far_row, k, :, lanes] += value

    for block in range(blocks - 1):
        add_far(block)

    @pl.when(jnp.logical_not(hub))
    def _():
        gather_sums.wait_send()
        share_sums.wait_recv()

    misfit[...] = total[:steps] / total[steps : steps + 1] - wanted[...]
    add_far(blocks - 1)

    arrive(multipliers.at[far_halo, pl.ds(1, steps - 1)], far_send.at[1])

    @pl.when(relay)
    def _():
        arrive(parcel, relay_sem.at[1])

    @pl.when(hub)
    def _():
        arrive(held.at[far_halo, pl.ds(0, steps)], far_send.at[0])
        arrive(gathered.at[:, pl.ds(0, steps + 1)], chain_sem.at[0])
        share_sums.wait_send()


def solve(count, state, adjoint, control, regions, target, mask):
    steps, rows, planes, width = control.shape
    count_regions = target.shape[1]
    padded = (steps + 8, count_regions)
    blocks = width // 128
    f32, dma, vmem = jnp.float32, pltpu.SemaphoreType.DMA, pltpu.VMEM
    in_vmem = pl.BlockSpec(memory_space=pltpu.VMEM)
    return pl.pallas_call(
        functools.partial(solve_kernel, count),
        out_shape=(
            vmem((2,) + control.shape, f32),
            vmem((rows, steps, planes, width), f32),
            vmem(control.shape, f32),
            vmem(target.shape, f32),
            vmem(regions.shape, jnp.int32),
            vmem((rows + 2, steps, planes, width), f32),
        ),
        in_specs=[HBM] * 6,
        out_specs=(in_vmem,) * 6,
        scratch_shapes=[
            vmem((rows, planes, steps, width), f32),
            vmem((rows + 2, steps + 1, planes, width), f32),
            vmem((rows, steps, planes, width), f32),
            vmem(target.shape, f32),
            pltpu.SMEM(mask.shape, jnp.int32),
            vmem((steps, planes, width), f32),
        ]
        + [vmem(padded, f32)] * 6
        + [
            vmem((count // 4 - 1,) + padded, f32),
            vmem((RELAY_STEPS, planes, 128), f32),
            dma((6,)),
            pltpu.SemaphoreType.REGULAR,
            dma((2,)),
            dma((2,)),
            dma((1 + blocks,)),
            dma((3,)),
            dma((2,)),
            dma((2,)),
        ],
        compiler_params=pltpu.CompilerParams(
            collective_id=0, has_side_effects=True, vmem_limit_bytes=24 * 2**20
        ),
        name="solve",
    )(state, adjoint, control, regions, target, mask)


def finish_kernel(
    state_buffer, packed, gradient, misfit, labels, multipliers,
    state_out, adjoint_out, gradient_out,
    adjoint_buffer, table, late, out_sem,
):
    steps, rows, planes, width = gradient.shape
    writes = [
        pltpu.make_async_copy(state_buffer, state_out, out_sem.at[0]),
        pltpu.make_async_copy(gradient, gradient_out, out_sem.at[1]),
    ]
    for write in writes:
        write.start()

    values = real_transform([jnp.broadcast_to(misfit[j : j + 1], (8, table.shape[2])) for j in range(steps)])
    for k, value in enumerate(pack(*values)):
        table[k] = value

    blocks = width // 128
    odd = lax.axis_index("space") % 2
    for k, value in enumerate(
        halo_transform(multipliers, odd * (rows + 1), pl.ds((blocks - 1) * 128, 128))
    ):
        late[0, k] = jnp.zeros_like(value)
        late[1, k] = value

    def row_body(y, carry):
        chosen = jnp.where(y == odd * (rows - 1), 1, 0)
        for block in range(blocks):
            lanes = pl.ds(block * 128, 128)
            ids = labels[y, :, lanes]
            values = [
                packed[y, k, :, lanes] + jnp.take_along_axis(table[k], ids, axis=1, mode="promise_in_bounds")
                for k in range(steps)
            ]
            if block == blocks - 1:
                values = [value + late[chosen, k] for k, value in enumerate(values)]
            top = steps // 2 + 1
            imag = [None] + values[top:] + [None] * (2 * top - 1 - steps)

            def put(part, k, value):
                adjoint_buffer[part, y, k, :, lanes] = value

            write_spectrum(put, values[:top], imag, steps)
        for part in range(2):
            pltpu.make_async_copy(
                adjoint_buffer.at[part, y], adjoint_out.at[part, pl.ds(0, steps), y], out_sem.at[2]
            ).start()
        return carry

    lax.fori_loop(0, rows, row_body, 0)
    for write in writes:
        write.wait()
    pltpu.make_async_copy(adjoint_buffer, adjoint_buffer, out_sem.at[2]).wait()


def finish(control, state_buffer, packed, gradient, misfit, labels, multipliers):
    steps, rows, planes, width = control.shape
    f32, dma = jnp.float32, pltpu.SemaphoreType.DMA
    in_vmem = pl.BlockSpec(memory_space=pltpu.VMEM)
    spectrum_shape = jax.ShapeDtypeStruct((2,) + control.shape, f32)
    return pl.pallas_call(
        finish_kernel,
        out_shape=(spectrum_shape, spectrum_shape, jax.ShapeDtypeStruct(control.shape, f32)),
        in_specs=[in_vmem] * 6,
        out_specs=(HBM,) * 3,
        scratch_shapes=[
            pltpu.VMEM((2, rows, steps, planes, width), f32),
            pltpu.VMEM((steps, 8, misfit.shape[1]), f32),
            pltpu.VMEM((2, steps, planes, 128), f32),
            dma((3,)),
        ],
        compiler_params=pltpu.CompilerParams(vmem_limit_bytes=16 * 2**20),
        name="finish",
    )(state_buffer, packed, gradient, misfit, labels, multipliers)


def on_device(count, *arrays):
    state, adjoint, control, target, mask, regions = (
        pltpu.with_memory_space_constraint(array, pltpu.HBM) for array in arrays
    )
    found = solve(count, state, adjoint, control, regions, target, mask)
    return finish(control, *found)


def solution(mesh):
    return jax.shard_map(
        functools.partial(on_device, mesh.shape["space"]),
        mesh=mesh,
        in_specs=(
            P("parts", "space", None, None),
            P("parts", "space", None, None),
            P("parts", "space", None, None),
            P("parts", None),
            P("space", "parts"),
            P("space", "parts", None),
        ),
        out_specs=(
            P(None, "parts", "space", None, None),
            P(None, "parts", "space", None, None),
            P("parts", "space", None, None),
        ),
        check_vma=False,
    )
```

```python
import functools
import math

import jax
import jax.numpy as jnp
from jax import lax
from jax.experimental import pallas as pl
from jax.experimental.pallas import tpu as pltpu
from jax.sharding import PartitionSpec as P

time_step = 0.15
penalty = 0.5
MESH = pl.DeviceIdType.MESH
HBM = pl.BlockSpec(memory_space=pltpu.HBM)
RELAY_STEPS = 5


def real_transform(values):
    n = len(values)
    if n == 1:
        return [values[0]], [None]
    if n % 2:
        real, imag = [], []
        for k in range(n // 2 + 1):
            angles = [2.0 * math.pi * (j * k % n) / n for j in range(n)]
            real.append(sum(v * math.cos(a) for v, a in zip(values, angles)))
            imag.append(None if k == 0 else sum(v * -math.sin(a) for v, a in zip(values, angles)))
        return real, imag
    even_re, even_im = real_transform(values[::2])
    odd_re, odd_im = real_transform(values[1::2])
    m = n // 2
    real, imag = [None] * (m + 1), [None] * (m + 1)
    for k in range(m // 2 + 1):
        a_re, a_im, b_re, b_im = even_re[k], even_im[k], odd_re[k], odd_im[k]
        if k == 0:
            real[0], real[m] = a_re + b_re, a_re - b_re
            continue
        if 2 * k == m:
            real[k], imag[k] = a_re, -b_re
            continue
        c, s = math.cos(2.0 * math.pi * k / n), math.sin(2.0 * math.pi * k / n)
        t_re, t_im = c * b_re + s * b_im, c * b_im - s * b_re
        real[k], imag[k] = a_re + t_re, a_im + t_im
        real[m - k], imag[m - k] = a_re - t_re, t_im - a_im
    return real, imag


def write_spectrum(put, real, imag, n):
    zero = jnp.zeros_like(real[0])
    for k in range(n):
        low = min(k, n - k)
        put(0, k, real[low])
        value = imag[low]
        put(1, k, zero if value is None else (value if k == low else -value))


def pack(real, imag):
    return real + [value for value in imag if value is not None]


def halo_transform(multipliers, halo, lanes):
    steps = multipliers.shape[1]
    values = [-time_step * multipliers[halo, j + 1, :, lanes] for j in range(steps - 1)]
    values.append(jnp.zeros_like(values[0]))
    return pack(*real_transform(values))


def solve_kernel(
    count, state, adjoint, control, regions, target, mask,
    state_buffer, packed, gradient, misfit, labels, multipliers,
    sampled, held, heat, wanted, allowed, residual, partial, paired, joined, crossed, summed, total, gathered, parcel,
    load_sem, ready, near_sem, far_send, far_recv, sum_sem, chain_sem, relay_sem,
):
    steps, rows, planes, width = control.shape
    count_regions = target.shape[1]
    blocks = width // 128
    links = count // 4
    me = lax.axis_index("space")
    link, place = me // 4, me % 4
    odd = me % 2
    partner = me + 1 - 2 * odd
    outside = (me + count - 1 + 2 * odd) % count
    hub = (place == 0) | (place == 3)
    last = me == count - 1
    origin = me == 0
    relays = min(links - 1, 3)
    carried = RELAY_STEPS
    direct = steps - 1 - relays * carried
    relay = (place == 0) & (link >= 1) & (link <= relays)
    helpers = [4 * (d + 1) for d in range(relays) if d + 1 < links - 1]
    mate = link * 4 + 3 - place
    peers = [((link + d) % links) * 4 + place for d in range(1, links)]
    near_row, far_row = (1 - odd) * (rows - 1), odd * (rows - 1)
    near_halo, far_halo = (1 - odd) * (rows + 1), odd * (rows + 1)

    barrier = pltpu.get_barrier_semaphore()

    def greet(other):
        pl.semaphore_signal(barrier, inc=1, device_id={"space": other}, device_id_type=MESH)

    greet(partner)
    greet(outside)

    @pl.when(hub)
    def _():
        for other in [mate] + peers:
            greet(other)

    @pl.when(relay & (link < links - 1))
    def _():
        greet(count - 1)

    label_load = pltpu.make_async_copy(regions, labels, load_sem.at[0])

    def local(source, into, sem):
        return pltpu.make_async_copy(source, into, sem)

    sample_loads = [
        local(state.at[pl.ds(1, steps), y, plane], sampled.at[y, plane], load_sem.at[0])
        for y in range(rows)
        for plane in range(planes)
    ]
    later_loads = [local(mask, allowed, load_sem.at[1]), local(target, wanted, load_sem.at[2])]
    own = pl.ds(1, rows)
    for y in range(rows):
        later_loads += [
            local(adjoint.at[pl.ds(0, steps), y], multipliers.at[y + 1], load_sem.at[3]),
            local(control.at[pl.ds(0, steps), y], heat.at[y], load_sem.at[4]),
            local(state.at[pl.ds(0, steps + 1), y], held.at[y + 1], load_sem.at[5]),
        ]
    def arrive(ref, sem):
        local(ref, ref, sem).wait()

    def arrive_slabs(count, sem):
        arrive(held.reshape((rows + 2) * (steps + 1), planes, width).at[pl.ds(0, count)], sem)

    near_copies, far_copies = [], []
    for source, first, target_rows, shift, length in (
        (state, 0, held, 0, steps), (adjoint, 1, multipliers, 1, steps - 1),
    ):
        n = len(near_copies)
        near_copies.append(
            pltpu.make_async_remote_copy(
                src_ref=source.at[pl.ds(first, length), near_row],
                dst_ref=target_rows.at[odd * (rows + 1), pl.ds(shift, length)],
                send_sem=near_sem.at[0],
                recv_sem=near_sem.at[1],
                device_id={"space": partner},
                device_id_type=MESH,
            )
        )
        for block in range(blocks):
            lanes = pl.ds(block * 128, 128)
            n = len(far_copies)
            far_copies.append(
                pltpu.make_async_remote_copy(
                    src_ref=source.at[pl.ds(first, length), far_row, :, lanes],
                    dst_ref=target_rows.at[(1 - odd) * (rows + 1), pl.ds(shift, length), :, lanes],
                    send_sem=far_send.at[n // blocks],
                    recv_sem=far_recv.at[max(n - blocks + 1, 0)],
                    device_id={"space": outside},
                    device_id_type=MESH,
                )
            )

    lanes = pl.ds((blocks - 1) * 128, 128)
    short_copy = pltpu.make_async_remote_copy(
        src_ref=adjoint.at[pl.ds(1, direct), far_row, :, lanes],
        dst_ref=multipliers.at[(1 - odd) * (rows + 1), pl.ds(1, direct), :, lanes],
        send_sem=far_send.at[1],
        recv_sem=far_recv.at[blocks],
        device_id={"space": outside},
        device_id_type=MESH,
    )
    relay_out = [
        pltpu.make_async_remote_copy(
            src_ref=adjoint.at[pl.ds(1 + direct + d * carried, carried), far_row, :, lanes],
            dst_ref=parcel,
            send_sem=far_send.at[1],
            recv_sem=relay_sem.at[0],
            device_id={"space": jnp.int32(4 * (d + 1))},
            device_id_type=MESH,
        )
        for d in range(relays)
    ]
    relay_on = pltpu.make_async_remote_copy(
        src_ref=parcel,
        dst_ref=multipliers.at[0, pl.ds(1 + direct + (link + relays - 1) % relays * carried, carried), :, lanes],
        send_sem=relay_sem.at[1],
        recv_sem=relay_sem.at[0],
        device_id={"space": jnp.int32(0)},
        device_id_type=MESH,
    )

    def message(n, source, into, other):
        source, into = source.at[pl.ds(0, steps + 1)], into.at[pl.ds(0, steps + 1)]
        return pltpu.make_async_remote_copy(
            src_ref=source, dst_ref=into, send_sem=sum_sem.at[0], recv_sem=sum_sem.at[1 + n % 2],
            device_id={"space": other}, device_id_type=MESH,
        )

    gather_sums = message(0, partial, paired, partner)
    cross_sums = message(1, joined, crossed, mate)
    share_sums = message(2, total, total, partner)
    chain_sums = [
        pltpu.make_async_remote_copy(
            src_ref=summed.at[pl.ds(0, steps + 1)], dst_ref=gathered.at[d, pl.ds(0, steps + 1)], send_sem=chain_sem.at[0], recv_sem=chain_sem.at[1],
            device_id={"space": peer}, device_id_type=MESH,
        )
        for d, peer in enumerate(peers)
    ]

    region_ids = lax.broadcasted_iota(jnp.int32, (count_regions, width), 0).astype(jnp.float32).astype(jnp.bfloat16)
    yes = jnp.ones((count_regions, width), jnp.bfloat16)
    no = jnp.zeros((count_regions, width), jnp.bfloat16)

    def add_row(row, carry):
        values = jnp.concatenate([sampled[row, plane] for plane in range(planes)], axis=1)
        high = values.astype(jnp.bfloat16)
        low = (values - high.astype(jnp.float32)).astype(jnp.bfloat16)
        ones = jnp.ones((16, planes * width), jnp.bfloat16)
        stacked = jnp.concatenate([high, low, ones], axis=0)
        onehot = jnp.concatenate(
            [
                jnp.where(
                    labels[row, pl.ds(plane, 1), :].astype(jnp.float32).astype(jnp.bfloat16) == region_ids, yes, no
                )
                for plane in range(planes)
            ],
            axis=1,
        )
        return carry + lax.dot_general(
            stacked, onehot, (((1,), (1,)), ((), ())), preferred_element_type=jnp.float32
        )

    def meet():
        pl.semaphore_wait(barrier, 2)
        for copy in far_copies:
            copy.start()
        pl.semaphore_signal(ready, inc=1, device_id={"space": outside}, device_id_type=MESH)

    pl.when(place == 2)(meet)
    label_load.start()
    for load in sample_loads:
        load.start()
    pl.when(place == 1)(meet)

    arrive_slabs(rows * (steps + 1), load_sem.at[0])
    found = jnp.zeros((2 * steps + 16, count_regions), jnp.float32)
    for y in range(rows):
        found = add_row(y, found)
    partial[:steps] = found[:steps] + found[steps : 2 * steps]
    partial[steps:] = found[2 * steps : 2 * steps + 8]

    @pl.when(jnp.logical_not(hub))
    def _():
        pl.semaphore_wait(ready, 1)
        gather_sums.start()
        for copy in near_copies:
            copy.start()
        arrive(held.at[far_halo, pl.ds(0, steps)], far_send.at[0])

    for load in later_loads:
        load.start()

    @pl.when(last)
    def _():
        pl.semaphore_wait(barrier, 3 + len(peers) + len(helpers))
        for copy in relay_out + far_copies[:-1] + [short_copy]:
            copy.start()

    @pl.when(hub)
    def _():
        gather_sums.wait_recv()
        joined[...] = partial[...] + paired[...]
        cross_sums.start()
        for copy in near_copies:
            copy.start()

        @pl.when(jnp.logical_not(last | origin))
        def _():
            pl.semaphore_wait(barrier, 3 + len(peers))

        @pl.when((place == 0) & jnp.logical_not(origin))
        def _():
            for copy in far_copies[:blocks]:
                copy.start()

    lane = lax.broadcasted_iota(jnp.int32, (planes, width), 1)
    plane_ids = lax.broadcasted_iota(jnp.int32, (planes, width), 0)
    first_lane, last_lane = lane == 0, lane == width - 1
    first_plane, last_plane = plane_ids == 0, plane_ids == planes - 1

    def support_of(y):
        support = jnp.zeros((planes, width), jnp.float32)
        for plane in range(planes):
            support = jnp.where(plane_ids == plane, allowed[y, plane].astype(jnp.float32), support)
        return support

    def laplace(values, beside):
        total = beside + jnp.where(first_lane, 0.0, pltpu.roll(values, 1, 1))
        total = total + jnp.where(last_lane, 0.0, pltpu.roll(values, width - 1, 1))
        total = total + jnp.where(first_plane, 0.0, pltpu.roll(values, 1, 0))
        total = total + jnp.where(last_plane, 0.0, pltpu.roll(values, planes - 1, 0))
        return total - 6.0 * values

    def adjoint_transform(y, beside):
        def step(j, carry):
            later = multipliers[y + 1, j + 1]
            residual[j] = multipliers[y + 1, j] - later - time_step * laplace(later, beside(j + 1))
            return carry

        lax.fori_loop(0, steps - 1, step, 0, unroll=True)
        residual[steps - 1] = multipliers[y + 1, steps - 1]
        for block in range(blocks):
            lanes = pl.ds(block * 128, 128)
            values = real_transform([residual[j, :, lanes] for j in range(steps)])
            for k, value in enumerate(pack(*values)):
                packed[y, k, :, lanes] = value

    def adjoint_full(y, carry):
        adjoint_transform(y, lambda j: multipliers[y, j] + multipliers[y + 2, j])
        return carry

    def state_row(y, carry):
        support = support_of(y)

        def step(j, inner):
            now = held[y + 1, j]
            lap = laplace(now, held[y, j] + held[y + 2, j])
            residual[j] = held[y + 1, j + 1] - now - time_step * lap - time_step * support * heat[y, j]
            return inner

        lax.fori_loop(0, steps, step, 0, unroll=True)
        for block in range(blocks):
            lanes = pl.ds(block * 128, 128)
            real, imag = real_transform([residual[j, :, lanes] for j in range(steps)])

            def put(part, k, value):
                state_buffer[part, k, y, :, lanes] = value

            write_spectrum(put, real, imag, steps)
        return carry

    def gradient_row(y, carry):
        support = support_of(y)

        def step(j, inner):
            gradient[j, y] = penalty * heat[y, j] - support * multipliers[y + 1, j]
            return inner

        return lax.fori_loop(0, steps, step, carry, unroll=True)

    for load in later_loads[:2]:
        load.wait()
    arrive(multipliers.at[own], load_sem.at[3])
    arrive(heat, load_sem.at[4])
    arrive(held.at[own], load_sem.at[5])

    lax.fori_loop(1, rows - 1, adjoint_full, 0)

    adjoint_transform(far_row, lambda j: multipliers[far_row + 2 - 2 * odd, j])

    lax.fori_loop(0, rows, gradient_row, 0)

    @pl.when(origin)
    def _():
        pl.semaphore_wait(barrier, 3 + len(peers))
        far_copies[0].start()

    @pl.when(hub)
    def _():
        cross_sums.wait()
        summed[...] = joined[...] + crossed[...]
        for send in chain_sums:
            send.start()

        @pl.when(relay)
        def _():
            arrive(parcel, relay_sem.at[0])
            relay_on.start()

        @pl.when(jnp.logical_not(last | origin))
        def _():
            @pl.when(place == 0)
            def _():
                for copy in far_copies[blocks:]:
                    copy.start()

    lax.fori_loop(1, rows - 1, state_row, 0)

    @pl.when((place == 3) & jnp.logical_not(last))
    def _():
        for copy in far_copies:
            copy.start()


    arrive_slabs(2 * steps - 1, near_sem.at[0])
    arrive_slabs(2 * steps - 1, near_sem.at[1])
    lax.fori_loop(near_row, near_row + 1, adjoint_full, 0)
    lax.fori_loop(near_row, near_row + 1, state_row, 0)

    @pl.when(origin)
    def _():
        for copy in far_copies[1:]:
            copy.start()

    @pl.when(hub)
    def _():
        result = summed[...]
        arrive(gathered.at[:, pl.ds(0, steps + 1)], chain_sem.at[1])
        for d in range(len(peers)):
            result = result + gathered[d]
        total[...] = result
        share_sums.start()

    arrive(held.at[far_halo, pl.ds(0, steps)], far_recv.at[0])
    lax.fori_loop(far_row, far_row + 1, state_row, 0)

    def add_far(block):
        lanes = pl.ds(block * 128, 128)
        if block < blocks - 1:
            far_copies[blocks + block].wait_recv()
        else:
            pl.when(jnp.logical_not(origin))(far_copies[-1].wait_recv)

            @pl.when(origin)
            def _():
                short_copy.wait_recv()
                arrive(multipliers.at[0, pl.ds(1 + direct, relays * carried), :, lanes], relay_sem.at[0])

        if block < blocks - 1:
            for k, value in enumerate(halo_transform(multipliers, far_halo, lanes)):
                packed[far_row, k, :, lanes] += value

    for block in range(blocks - 1):
        add_far(block)

    @pl.when(jnp.logical_not(hub))
    def _():
        gather_sums.wait_send()
        share_sums.wait_recv()

    misfit[...] = total[:steps] / total[steps : steps + 1] - wanted[...]
    add_far(blocks - 1)

    arrive(multipliers.at[far_halo, pl.ds(1, steps - 1)], far_send.at[1])

    @pl.when(relay)
    def _():
        arrive(parcel, relay_sem.at[1])

    @pl.when(hub)
    def _():
        arrive(held.at[far_halo, pl.ds(0, steps)], far_send.at[0])
        arrive(gathered.at[:, pl.ds(0, steps + 1)], chain_sem.at[0])
        share_sums.wait_send()


def solve(count, state, adjoint, control, regions, target, mask):
    steps, rows, planes, width = control.shape
    count_regions = target.shape[1]
    padded = (steps + 8, count_regions)
    blocks = width // 128
    f32, dma, vmem = jnp.float32, pltpu.SemaphoreType.DMA, pltpu.VMEM
    in_vmem = pl.BlockSpec(memory_space=pltpu.VMEM)
    return pl.pallas_call(
        functools.partial(solve_kernel, count),
        out_shape=(
            vmem((2,) + control.shape, f32),
            vmem((rows, steps, planes, width), f32),
            vmem(control.shape, f32),
            vmem(target.shape, f32),
            vmem(regions.shape, jnp.int32),
            vmem((rows + 2, steps, planes, width), f32),
        ),
        in_specs=[HBM] * 6,
        out_specs=(in_vmem,) * 6,
        scratch_shapes=[
            vmem((rows, planes, steps, width), f32),
            vmem((rows + 2, steps + 1, planes, width), f32),
            vmem((rows, steps, planes, width), f32),
            vmem(target.shape, f32),
            pltpu.SMEM(mask.shape, jnp.int32),
            vmem((steps, planes, width), f32),
        ]
        + [vmem(padded, f32)] * 6
        + [
            vmem((count // 4 - 1,) + padded, f32),
            vmem((RELAY_STEPS, planes, 128), f32),
            dma((6,)),
            pltpu.SemaphoreType.REGULAR,
            dma((2,)),
            dma((2,)),
            dma((1 + blocks,)),
            dma((3,)),
            dma((2,)),
            dma((2,)),
        ],
        compiler_params=pltpu.CompilerParams(
            collective_id=0, has_side_effects=True, vmem_limit_bytes=24 * 2**20
        ),
        name="solve",
    )(state, adjoint, control, regions, target, mask)


def finish_kernel(
    state_buffer, packed, gradient, misfit, labels, multipliers,
    state_out, adjoint_out, gradient_out,
    adjoint_buffer, table, late, out_sem,
):
    steps, rows, planes, width = gradient.shape
    writes = [
        pltpu.make_async_copy(gradient, gradient_out, out_sem.at[1]),
        pltpu.make_async_copy(state_buffer, state_out, out_sem.at[0]),
    ]
    for write in writes:
        write.start()

    values = real_transform([jnp.broadcast_to(misfit[j : j + 1], (8, table.shape[2])) for j in range(steps)])
    for k, value in enumerate(pack(*values)):
        table[k] = value

    blocks = width // 128
    odd = lax.axis_index("space") % 2
    for k, value in enumerate(
        halo_transform(multipliers, odd * (rows + 1), pl.ds((blocks - 1) * 128, 128))
    ):
        late[0, k] = jnp.zeros_like(value)
        late[1, k] = value

    def row_body(y, carry):
        chosen = jnp.where(y == odd * (rows - 1), 1, 0)
        for block in range(blocks):
            lanes = pl.ds(block * 128, 128)
            ids = labels[y, :, lanes]
            values = [
                packed[y, k, :, lanes] + jnp.take_along_axis(table[k], ids, axis=1, mode="promise_in_bounds")
                for k in range(steps)
            ]
            if block == blocks - 1:
                values = [value + late[chosen, k] for k, value in enumerate(values)]
            top = steps // 2 + 1
            imag = [None] + values[top:] + [None] * (2 * top - 1 - steps)

            def put(part, k, value):
                adjoint_buffer[part, y, k, :, lanes] = value

            write_spectrum(put, values[:top], imag, steps)
        for part in range(2):
            pltpu.make_async_copy(
                adjoint_buffer.at[part, y], adjoint_out.at[part, pl.ds(0, steps), y], out_sem.at[2]
            ).start()
        return carry

    lax.fori_loop(0, rows, row_body, 0)
    for write in writes:
        write.wait()
    pltpu.make_async_copy(adjoint_buffer, adjoint_buffer, out_sem.at[2]).wait()


def finish(control, state_buffer, packed, gradient, misfit, labels, multipliers):
    steps, rows, planes, width = control.shape
    f32, dma = jnp.float32, pltpu.SemaphoreType.DMA
    in_vmem = pl.BlockSpec(memory_space=pltpu.VMEM)
    spectrum_shape = jax.ShapeDtypeStruct((2,) + control.shape, f32)
    return pl.pallas_call(
        finish_kernel,
        out_shape=(spectrum_shape, spectrum_shape, jax.ShapeDtypeStruct(control.shape, f32)),
        in_specs=[in_vmem] * 6,
        out_specs=(HBM,) * 3,
        scratch_shapes=[
            pltpu.VMEM((2, rows, steps, planes, width), f32),
            pltpu.VMEM((steps, 8, misfit.shape[1]), f32),
            pltpu.VMEM((2, steps, planes, 128), f32),
            dma((3,)),
        ],
        compiler_params=pltpu.CompilerParams(vmem_limit_bytes=16 * 2**20),
        name="finish",
    )(state_buffer, packed, gradient, misfit, labels, multipliers)


def on_device(count, *arrays):
    state, adjoint, control, target, mask, regions = (
        pltpu.with_memory_space_constraint(array, pltpu.HBM) for array in arrays
    )
    found = solve(count, state, adjoint, control, regions, target, mask)
    return finish(control, *found)


def solution(mesh):
    return jax.shard_map(
        functools.partial(on_device, mesh.shape["space"]),
        mesh=mesh,
        in_specs=(
            P("parts", "space", None, None),
            P("parts", "space", None, None),
            P("parts", "space", None, None),
            P("parts", None),
            P("space", "parts"),
            P("space", "parts", None),
        ),
        out_specs=(
            P(None, "parts", "space", None, None),
            P(None, "parts", "space", None, None),
            P("parts", "space", None, None),
        ),
        check_vma=False,
    )
```

```python
import functools
import math

import jax
import jax.numpy as jnp
from jax import lax
from jax.experimental import pallas as pl
from jax.experimental.pallas import tpu as pltpu
from jax.sharding import PartitionSpec as P

time_step = 0.15
penalty = 0.5
MESH = pl.DeviceIdType.MESH
HBM = pl.BlockSpec(memory_space=pltpu.HBM)
RELAY_STEPS = 5


def real_transform(values):
    n = len(values)
    if n == 1:
        return [values[0]], [None]
    if n % 2:
        real, imag = [], []
        for k in range(n // 2 + 1):
            angles = [2.0 * math.pi * (j * k % n) / n for j in range(n)]
            real.append(sum(v * math.cos(a) for v, a in zip(values, angles)))
            imag.append(None if k == 0 else sum(v * -math.sin(a) for v, a in zip(values, angles)))
        return real, imag
    even_re, even_im = real_transform(values[::2])
    odd_re, odd_im = real_transform(values[1::2])
    m = n // 2
    real, imag = [None] * (m + 1), [None] * (m + 1)
    for k in range(m // 2 + 1):
        a_re, a_im, b_re, b_im = even_re[k], even_im[k], odd_re[k], odd_im[k]
        if k == 0:
            real[0], real[m] = a_re + b_re, a_re - b_re
            continue
        if 2 * k == m:
            real[k], imag[k] = a_re, -b_re
            continue
        c, s = math.cos(2.0 * math.pi * k / n), math.sin(2.0 * math.pi * k / n)
        t_re, t_im = c * b_re + s * b_im, c * b_im - s * b_re
        real[k], imag[k] = a_re + t_re, a_im + t_im
        real[m - k], imag[m - k] = a_re - t_re, t_im - a_im
    return real, imag


def write_spectrum(put, real, imag, n):
    zero = jnp.zeros_like(real[0])
    for k in range(n):
        low = min(k, n - k)
        put(0, k, real[low])
        value = imag[low]
        put(1, k, zero if value is None else (value if k == low else -value))


def pack(real, imag):
    return real + [value for value in imag if value is not None]


def halo_transform(multipliers, halo, lanes):
    steps = multipliers.shape[1]
    values = [-time_step * multipliers[halo, j + 1, :, lanes] for j in range(steps - 1)]
    values.append(jnp.zeros_like(values[0]))
    return pack(*real_transform(values))


def solve_kernel(
    count, state, adjoint, control, regions, target, mask,
    state_buffer, packed, gradient, misfit, labels, multipliers,
    sampled, held, heat, wanted, allowed, residual, partial, paired, joined, crossed, summed, total, gathered, parcel,
    load_sem, ready, near_sem, far_send, far_recv, sum_sem, chain_sem, relay_sem,
):
    steps, rows, planes, width = control.shape
    count_regions = target.shape[1]
    blocks = width // 128
    links = count // 4
    me = lax.axis_index("space")
    link, place = me // 4, me % 4
    odd = me % 2
    partner = me + 1 - 2 * odd
    outside = (me + count - 1 + 2 * odd) % count
    hub = (place == 0) | (place == 3)
    last = me == count - 1
    origin = me == 0
    relays = min(links - 1, 3)
    carried = RELAY_STEPS
    direct = steps - 1 - relays * carried
    relay = (place == 0) & (link >= 1) & (link <= relays)
    helpers = [4 * (d + 1) for d in range(relays) if d + 1 < links - 1]
    mate = link * 4 + 3 - place
    peers = [((link + d) % links) * 4 + place for d in range(1, links)]
    near_row, far_row = (1 - odd) * (rows - 1), odd * (rows - 1)
    near_halo, far_halo = (1 - odd) * (rows + 1), odd * (rows + 1)

    barrier = pltpu.get_barrier_semaphore()

    def greet(other):
        pl.semaphore_signal(barrier, inc=1, device_id={"space": other}, device_id_type=MESH)

    greet(partner)
    greet(outside)

    @pl.when(hub)
    def _():
        for other in [mate] + peers:
            greet(other)

    @pl.when(relay & (link < links - 1))
    def _():
        greet(count - 1)

    label_load = pltpu.make_async_copy(regions, labels, load_sem.at[0])

    def local(source, into, sem):
        return pltpu.make_async_copy(source, into, sem)

    sample_loads = [
        local(state.at[pl.ds(1, steps), y, plane], sampled.at[y, plane], load_sem.at[0])
        for y in range(rows)
        for plane in range(planes)
    ]
    later_loads = [local(mask, allowed, load_sem.at[1]), local(target, wanted, load_sem.at[2])]
    own = pl.ds(1, rows)
    for y in range(rows):
        later_loads += [
            local(adjoint.at[pl.ds(0, steps), y], multipliers.at[y + 1], load_sem.at[3]),
            local(control.at[pl.ds(0, steps), y], heat.at[y], load_sem.at[4]),
            local(state.at[pl.ds(0, steps + 1), y], held.at[y + 1], load_sem.at[5]),
        ]
    def arrive(ref, sem):
        local(ref, ref, sem).wait()

    def arrive_slabs(count, sem):
        arrive(held.reshape((rows + 2) * (steps + 1), planes, width).at[pl.ds(0, count)], sem)

    near_copies, far_copies = [], []
    for source, first, target_rows, shift, length in (
        (state, 0, held, 0, steps), (adjoint, 1, multipliers, 1, steps - 1),
    ):
        n = len(near_copies)
        near_copies.append(
            pltpu.make_async_remote_copy(
                src_ref=source.at[pl.ds(first, length), near_row],
                dst_ref=target_rows.at[odd * (rows + 1), pl.ds(shift, length)],
                send_sem=far_send.at[1],
                recv_sem=near_sem.at[0],
                device_id={"space": partner},
                device_id_type=MESH,
            )
        )
        for block in range(blocks):
            lanes = pl.ds(block * 128, 128)
            n = len(far_copies)
            far_copies.append(
                pltpu.make_async_remote_copy(
                    src_ref=source.at[pl.ds(first, length), far_row, :, lanes],
                    dst_ref=target_rows.at[(1 - odd) * (rows + 1), pl.ds(shift, length), :, lanes],
                    send_sem=far_send.at[n // blocks],
                    recv_sem=far_recv.at[max(n - blocks + 1, 0)],
                    device_id={"space": outside},
                    device_id_type=MESH,
                )
            )

    lanes = pl.ds((blocks - 1) * 128, 128)
    short_copy = pltpu.make_async_remote_copy(
        src_ref=adjoint.at[pl.ds(1, direct), far_row, :, lanes],
        dst_ref=multipliers.at[(1 - odd) * (rows + 1), pl.ds(1, direct), :, lanes],
        send_sem=far_send.at[1],
        recv_sem=far_recv.at[blocks],
        device_id={"space": outside},
        device_id_type=MESH,
    )
    relay_out = [
        pltpu.make_async_remote_copy(
            src_ref=adjoint.at[pl.ds(1 + direct + d * carried, carried), far_row, :, lanes],
            dst_ref=parcel,
            send_sem=far_send.at[1],
            recv_sem=relay_sem.at[0],
            device_id={"space": jnp.int32(4 * (d + 1))},
            device_id_type=MESH,
        )
        for d in range(relays)
    ]
    relay_on = pltpu.make_async_remote_copy(
        src_ref=parcel,
        dst_ref=multipliers.at[0, pl.ds(1 + direct + (link + relays - 1) % relays * carried, carried), :, lanes],
        send_sem=relay_sem.at[1],
        recv_sem=relay_sem.at[0],
        device_id={"space": jnp.int32(0)},
        device_id_type=MESH,
    )

    def message(n, source, into, other):
        source, into = source.at[pl.ds(0, steps + 1)], into.at[pl.ds(0, steps + 1)]
        return pltpu.make_async_remote_copy(
            src_ref=source, dst_ref=into, send_sem=sum_sem.at[0], recv_sem=sum_sem.at[1 + n % 2],
            device_id={"space": other}, device_id_type=MESH,
        )

    gather_sums = message(0, partial, paired, partner)
    cross_sums = message(1, joined, crossed, mate)
    share_sums = message(2, total, total, partner)
    chain_sums = [
        pltpu.make_async_remote_copy(
            src_ref=summed.at[pl.ds(0, steps + 1)], dst_ref=gathered.at[d, pl.ds(0, steps + 1)], send_sem=chain_sem.at[0], recv_sem=chain_sem.at[1],
            device_id={"space": peer}, device_id_type=MESH,
        )
        for d, peer in enumerate(peers)
    ]

    region_ids = lax.broadcasted_iota(jnp.int32, (count_regions, width), 0).astype(jnp.float32).astype(jnp.bfloat16)
    yes = jnp.ones((count_regions, width), jnp.bfloat16)
    no = jnp.zeros((count_regions, width), jnp.bfloat16)

    def add_row(row, carry):
        values = jnp.concatenate([sampled[row, plane] for plane in range(planes)], axis=1)
        high = values.astype(jnp.bfloat16)
        low = (values - high.astype(jnp.float32)).astype(jnp.bfloat16)
        ones = jnp.ones((16, planes * width), jnp.bfloat16)
        stacked = jnp.concatenate([high, low, ones], axis=0)
        onehot = jnp.concatenate(
            [
                jnp.where(
                    labels[row, pl.ds(plane, 1), :].astype(jnp.float32).astype(jnp.bfloat16) == region_ids, yes, no
                )
                for plane in range(planes)
            ],
            axis=1,
        )
        return carry + lax.dot_general(
            stacked, onehot, (((1,), (1,)), ((), ())), preferred_element_type=jnp.float32
        )

    def meet():
        pl.semaphore_wait(barrier, 2)
        for copy in far_copies:
            copy.start()
        pl.semaphore_signal(ready, inc=1, device_id={"space": outside}, device_id_type=MESH)

    pl.when(place == 2)(meet)
    label_load.start()
    for load in sample_loads:
        load.start()
    pl.when(place == 1)(meet)

    arrive_slabs(rows * (steps + 1), load_sem.at[0])
    found = jnp.zeros((2 * steps + 16, count_regions), jnp.float32)
    for y in range(rows):
        found = add_row(y, found)
    partial[:steps] = found[:steps] + found[steps : 2 * steps]
    partial[steps:] = found[2 * steps : 2 * steps + 8]

    @pl.when(jnp.logical_not(hub))
    def _():
        pl.semaphore_wait(ready, 1)
        gather_sums.start()
        for copy in near_copies:
            copy.start()
        arrive(held.at[far_halo, pl.ds(0, steps)], far_send.at[0])

    for load in later_loads:
        load.start()

    @pl.when(last)
    def _():
        pl.semaphore_wait(barrier, 3 + len(peers) + len(helpers))
        for copy in relay_out + far_copies[:-1] + [short_copy]:
            copy.start()

    @pl.when(hub)
    def _():
        gather_sums.wait_recv()
        joined[...] = partial[...] + paired[...]
        cross_sums.start()
        for copy in near_copies:
            copy.start()

        @pl.when(jnp.logical_not(last | origin))
        def _():
            pl.semaphore_wait(barrier, 3 + len(peers))

        @pl.when((place == 0) & jnp.logical_not(origin))
        def _():
            for copy in far_copies[:blocks]:
                copy.start()

    lane = lax.broadcasted_iota(jnp.int32, (planes, width), 1)
    plane_ids = lax.broadcasted_iota(jnp.int32, (planes, width), 0)
    first_lane, last_lane = lane == 0, lane == width - 1
    first_plane, last_plane = plane_ids == 0, plane_ids == planes - 1

    def support_of(y):
        support = jnp.zeros((planes, width), jnp.float32)
        for plane in range(planes):
            support = jnp.where(plane_ids == plane, allowed[y, plane].astype(jnp.float32), support)
        return support

    def laplace(values, beside):
        total = beside + jnp.where(first_lane, 0.0, pltpu.roll(values, 1, 1))
        total = total + jnp.where(last_lane, 0.0, pltpu.roll(values, width - 1, 1))
        total = total + jnp.where(first_plane, 0.0, pltpu.roll(values, 1, 0))
        total = total + jnp.where(last_plane, 0.0, pltpu.roll(values, planes - 1, 0))
        return total - 6.0 * values

    def adjoint_transform(y, beside):
        def step(j, carry):
            later = multipliers[y + 1, j + 1]
            residual[j] = multipliers[y + 1, j] - later - time_step * laplace(later, beside(j + 1))
            return carry

        lax.fori_loop(0, steps - 1, step, 0, unroll=True)
        residual[steps - 1] = multipliers[y + 1, steps - 1]
        for block in range(blocks):
            lanes = pl.ds(block * 128, 128)
            values = real_transform([residual[j, :, lanes] for j in range(steps)])
            for k, value in enumerate(pack(*values)):
                packed[y, k, :, lanes] = value

    def adjoint_full(y, carry):
        adjoint_transform(y, lambda j: multipliers[y, j] + multipliers[y + 2, j])
        return carry

    def state_row(y, carry):
        support = support_of(y)

        def step(j, inner):
            now = held[y + 1, j]
            lap = laplace(now, held[y, j] + held[y + 2, j])
            residual[j] = held[y + 1, j + 1] - now - time_step * lap - time_step * support * heat[y, j]
            return inner

        lax.fori_loop(0, steps, step, 0, unroll=True)
        for block in range(blocks):
            lanes = pl.ds(block * 128, 128)
            real, imag = real_transform([residual[j, :, lanes] for j in range(steps)])

            def put(part, k, value):
                state_buffer[part, k, y, :, lanes] = value

            write_spectrum(put, real, imag, steps)
        return carry

    def gradient_row(y, carry):
        support = support_of(y)

        def step(j, inner):
            gradient[j, y] = penalty * heat[y, j] - support * multipliers[y + 1, j]
            return inner

        return lax.fori_loop(0, steps, step, carry, unroll=True)

    for load in later_loads[:2]:
        load.wait()
    arrive(multipliers.at[own], load_sem.at[3])
    arrive(heat, load_sem.at[4])
    arrive(held.at[own], load_sem.at[5])

    lax.fori_loop(1, rows - 1, adjoint_full, 0)

    adjoint_transform(far_row, lambda j: multipliers[far_row + 2 - 2 * odd, j])

    lax.fori_loop(0, rows, gradient_row, 0)

    @pl.when(origin)
    def _():
        pl.semaphore_wait(barrier, 3 + len(peers))
        far_copies[0].start()

    @pl.when(hub)
    def _():
        cross_sums.wait()
        summed[...] = joined[...] + crossed[...]
        for send in chain_sums:
            send.start()

        @pl.when(relay)
        def _():
            arrive(parcel, relay_sem.at[0])
            relay_on.start()

        @pl.when(jnp.logical_not(last | origin))
        def _():
            @pl.when(place == 0)
            def _():
                for copy in far_copies[blocks:]:
                    copy.start()

    lax.fori_loop(1, rows - 1, state_row, 0)

    @pl.when((place == 3) & jnp.logical_not(last))
    def _():
        for copy in far_copies:
            copy.start()


    arrive_slabs(2 * steps - 1, near_sem.at[0])
    lax.fori_loop(near_row, near_row + 1, adjoint_full, 0)
    lax.fori_loop(near_row, near_row + 1, state_row, 0)

    @pl.when(origin)
    def _():
        for copy in far_copies[1:]:
            copy.start()

    @pl.when(hub)
    def _():
        result = summed[...]
        arrive(gathered.at[:, pl.ds(0, steps + 1)], chain_sem.at[1])
        for d in range(len(peers)):
            result = result + gathered[d]
        total[...] = result
        share_sums.start()

    arrive(held.at[far_halo, pl.ds(0, steps)], far_recv.at[0])
    lax.fori_loop(far_row, far_row + 1, state_row, 0)

    def add_far(block):
        lanes = pl.ds(block * 128, 128)
        if block < blocks - 1:
            far_copies[blocks + block].wait_recv()
        else:
            pl.when(jnp.logical_not(origin))(far_copies[-1].wait_recv)

            @pl.when(origin)
            def _():
                short_copy.wait_recv()
                arrive(multipliers.at[0, pl.ds(1 + direct, relays * carried), :, lanes], relay_sem.at[0])

        if block < blocks - 1:
            for k, value in enumerate(halo_transform(multipliers, far_halo, lanes)):
                packed[far_row, k, :, lanes] += value

    for block in range(blocks - 1):
        add_far(block)

    @pl.when(jnp.logical_not(hub))
    def _():
        gather_sums.wait_send()
        share_sums.wait_recv()

    misfit[...] = total[:steps] / total[steps : steps + 1] - wanted[...]
    add_far(blocks - 1)

    arrive_slabs(3 * steps - 2, far_send.at[1])

    @pl.when(relay)
    def _():
        arrive(parcel, relay_sem.at[1])

    @pl.when(hub)
    def _():
        arrive(held.at[far_halo, pl.ds(0, steps)], far_send.at[0])
        arrive(gathered.at[:, pl.ds(0, steps + 1)], chain_sem.at[0])
        share_sums.wait_send()


def solve(count, state, adjoint, control, regions, target, mask):
    steps, rows, planes, width = control.shape
    count_regions = target.shape[1]
    padded = (steps + 8, count_regions)
    blocks = width // 128
    f32, dma, vmem = jnp.float32, pltpu.SemaphoreType.DMA, pltpu.VMEM
    in_vmem = pl.BlockSpec(memory_space=pltpu.VMEM)
    return pl.pallas_call(
        functools.partial(solve_kernel, count),
        out_shape=(
            vmem((2,) + control.shape, f32),
            vmem((rows, steps, planes, width), f32),
            vmem(control.shape, f32),
            vmem(target.shape, f32),
            vmem(regions.shape, jnp.int32),
            vmem((rows + 2, steps, planes, width), f32),
        ),
        in_specs=[HBM] * 6,
        out_specs=(in_vmem,) * 6,
        scratch_shapes=[
            vmem((rows, planes, steps, width), f32),
            vmem((rows + 2, steps + 1, planes, width), f32),
            vmem((rows, steps, planes, width), f32),
            vmem(target.shape, f32),
            pltpu.SMEM(mask.shape, jnp.int32),
            vmem((steps, planes, width), f32),
        ]
        + [vmem(padded, f32)] * 6
        + [
            vmem((count // 4 - 1,) + padded, f32),
            vmem((RELAY_STEPS, planes, 128), f32),
            dma((6,)),
            pltpu.SemaphoreType.REGULAR,
            dma((1,)),
            dma((2,)),
            dma((1 + blocks,)),
            dma((3,)),
            dma((2,)),
            dma((2,)),
        ],
        compiler_params=pltpu.CompilerParams(
            collective_id=0, has_side_effects=True, vmem_limit_bytes=24 * 2**20
        ),
        name="solve",
    )(state, adjoint, control, regions, target, mask)


def finish_kernel(
    state_buffer, packed, gradient, misfit, labels, multipliers,
    state_out, adjoint_out, gradient_out,
    adjoint_buffer, table, late, out_sem,
):
    steps, rows, planes, width = gradient.shape
    writes = [
        pltpu.make_async_copy(gradient, gradient_out, out_sem.at[1]),
        pltpu.make_async_copy(state_buffer, state_out, out_sem.at[0]),
    ]
    for write in writes:
        write.start()

    values = real_transform([jnp.broadcast_to(misfit[j : j + 1], (8, table.shape[2])) for j in range(steps)])
    for k, value in enumerate(pack(*values)):
        table[k] = value

    blocks = width // 128
    odd = lax.axis_index("space") % 2
    for k, value in enumerate(
        halo_transform(multipliers, odd * (rows + 1), pl.ds((blocks - 1) * 128, 128))
    ):
        late[0, k] = jnp.zeros_like(value)
        late[1, k] = value

    def row_body(y, carry):
        chosen = jnp.where(y == odd * (rows - 1), 1, 0)
        for block in range(blocks):
            lanes = pl.ds(block * 128, 128)
            ids = labels[y, :, lanes]
            values = [
                packed[y, k, :, lanes] + jnp.take_along_axis(table[k], ids, axis=1, mode="promise_in_bounds")
                for k in range(steps)
            ]
            if block == blocks - 1:
                values = [value + late[chosen, k] for k, value in enumerate(values)]
            top = steps // 2 + 1
            imag = [None] + values[top:] + [None] * (2 * top - 1 - steps)

            def put(part, k, value):
                adjoint_buffer[part, y, k, :, lanes] = value

            write_spectrum(put, values[:top], imag, steps)
        for part in range(2):
            pltpu.make_async_copy(
                adjoint_buffer.at[part, y], adjoint_out.at[part, pl.ds(0, steps), y], out_sem.at[2]
            ).start()
        return carry

    lax.fori_loop(0, rows, row_body, 0)
    for write in writes:
        write.wait()
    pltpu.make_async_copy(adjoint_buffer, adjoint_buffer, out_sem.at[2]).wait()


def finish(control, state_buffer, packed, gradient, misfit, labels, multipliers):
    steps, rows, planes, width = control.shape
    f32, dma = jnp.float32, pltpu.SemaphoreType.DMA
    in_vmem = pl.BlockSpec(memory_space=pltpu.VMEM)
    spectrum_shape = jax.ShapeDtypeStruct((2,) + control.shape, f32)
    return pl.pallas_call(
        finish_kernel,
        out_shape=(spectrum_shape, spectrum_shape, jax.ShapeDtypeStruct(control.shape, f32)),
        in_specs=[in_vmem] * 6,
        out_specs=(HBM,) * 3,
        scratch_shapes=[
            pltpu.VMEM((2, rows, steps, planes, width), f32),
            pltpu.VMEM((steps, 8, misfit.shape[1]), f32),
            pltpu.VMEM((2, steps, planes, 128), f32),
            dma((3,)),
        ],
        compiler_params=pltpu.CompilerParams(vmem_limit_bytes=16 * 2**20),
        name="finish",
    )(state_buffer, packed, gradient, misfit, labels, multipliers)


def on_device(count, *arrays):
    state, adjoint, control, target, mask, regions = (
        pltpu.with_memory_space_constraint(array, pltpu.HBM) for array in arrays
    )
    found = solve(count, state, adjoint, control, regions, target, mask)
    return finish(control, *found)


def solution(mesh):
    return jax.shard_map(
        functools.partial(on_device, mesh.shape["space"]),
        mesh=mesh,
        in_specs=(
            P("parts", "space", None, None),
            P("parts", "space", None, None),
            P("parts", "space", None, None),
            P("parts", None),
            P("space", "parts"),
            P("space", "parts", None),
        ),
        out_specs=(
            P(None, "parts", "space", None, None),
            P(None, "parts", "space", None, None),
            P("parts", "space", None, None),
        ),
        check_vma=False,
    )
```
